16 devices in a mesh: data: 2 (over y, z), model: 8 (over x, core).
Axes of the slice: x: 4, y: 2, z: 1, core: 2. Of those that a mesh axis runs over, the one named last changes fastest.
The devices are a block of a 4x4x8 slice.
Arguments:
- x_in: bfloat16 [16, 256, 4096], P('data'), parts along dimension 0
- seg_ids: int32 [16, 256], P('data'), parts along dimension 0
- ln_gain: bfloat16 [4096], replicated
- w_qkv: bfloat16 [4096, 16, 3, 256], P(None, 'model')
- w_out: bfloat16 [16, 256, 4096], P('model')
- w_up: bfloat16 [4096, 16384], P(None, 'model')
- w_down: bfloat16 [16384, 4096], P('model')
- dy_in: bfloat16 [16, 256, 4096], P('data'), parts along dimension 0
Outputs:
- output 1: bfloat16 [16, 256, 4096], P('data'), parts along dimension 0
- output 2: bfloat16 [16, 256, 4096], P('data'), parts along dimension 0
- output 3: bfloat16 [8192], P('data'), parts along dimension 0
- output 4: bfloat16 [8192, 16, 3, 256], P('data', 'model'), parts along dimension 0
- output 5: bfloat16 [32, 256, 4096], P(('data', 'model')), parts along dimension 0
- output 6: bfloat16 [8192, 16384], P('data', 'model'), parts along dimension 0
- output 7: bfloat16 [32768, 4096], P(('data', 'model')), parts along dimension 0
There are 2 independent parts. The reference program is written for one: setup_inputs(seed, part) draws one part's arguments, and reference() takes and returns one part's arrays. A program takes and returns all parts, laid end to end along the dimension named above; an argument that names none is the same for every part.
All inputs are finite; a program needn't handle non-finite values.
Results may differ from the reference program's by a relative error of at most 0.0177377.
Values are sent between devices in bfloat16 or wider.
A program may use at most 768 MiB of HBM per device.

```python
import jax
import jax.numpy as jnp
from jax import lax

GROUP_ROWS = 8
SEQ_LEN = 256
HIDDEN = 4096
NUM_HEADS = 16
HEAD_DIM = 256
FFN_DIM = 16384
LN_EPS = 1e-5


def setup_inputs(seed: int = 0, part: int = 0) -> dict:
    part_key = jax.random.fold_in(jax.random.key(seed), part)
    key_x, key_seg, key_dy = jax.random.split(part_key, 3)
    key_gain, key_qkv, key_out, key_up, key_down = jax.random.split(jax.random.key(seed + 1), 5)
    attn_width = NUM_HEADS * HEAD_DIM
    cuts = jax.random.randint(key_seg, (GROUP_ROWS, 3), 1, SEQ_LEN)
    positions = jnp.arange(SEQ_LEN)
    seg_ids = jnp.sum(positions[None, :, None] >= cuts[:, None, :], axis=-1).astype(jnp.int32)
    x_in = jax.random.normal(key_x, (GROUP_ROWS, SEQ_LEN, HIDDEN), jnp.float32)
    ln_gain = 1.0 + 0.3 * jax.random.normal(key_gain, (HIDDEN,), jnp.float32)
    w_qkv = jax.random.normal(key_qkv, (HIDDEN, NUM_HEADS, 3, HEAD_DIM), jnp.float32) * HIDDEN ** -0.5
    w_out = jax.random.normal(key_out, (NUM_HEADS, HEAD_DIM, HIDDEN), jnp.float32) * (3.0 * attn_width ** -0.5)
    w_up = jax.random.normal(key_up, (HIDDEN, FFN_DIM), jnp.float32) * HIDDEN ** -0.5
    w_down = jax.random.normal(key_down, (FFN_DIM, HIDDEN), jnp.float32) * FFN_DIM ** -0.5
    dy_in = jax.random.normal(key_dy, (GROUP_ROWS, SEQ_LEN, HIDDEN), jnp.float32)
    return {
        'x_in': x_in.astype(jnp.bfloat16),
        'seg_ids': seg_ids,
        'ln_gain': ln_gain.astype(jnp.bfloat16),
        'w_qkv': w_qkv.astype(jnp.bfloat16),
        'w_out': w_out.astype(jnp.bfloat16),
        'w_up': w_up.astype(jnp.bfloat16),
        'w_down': w_down.astype(jnp.bfloat16),
        'dy_in': dy_in.astype(jnp.bfloat16),
    }


def layer_norm(x_f32, ln_gain):
    mean_val = jnp.mean(x_f32, axis=-1, keepdims=True)
    centered = x_f32 - mean_val
    var_val = jnp.mean(centered * centered, axis=-1, keepdims=True)
    normed = centered * lax.rsqrt(var_val + LN_EPS)
    return (normed * ln_gain.astype(jnp.float32)).astype(jnp.bfloat16)


def head_attention(head_args):
    qkv_head, seg_row = head_args
    query = qkv_head[0]
    keys = qkv_head[1]
    values = qkv_head[2]
    scores = jnp.dot(query, keys.T, preferred_element_type=jnp.float32) * (HEAD_DIM ** -0.5)
    positions = jnp.arange(SEQ_LEN)
    allowed = (positions[None, :] <= positions[:, None]) & (seg_row[None, :] == seg_row[:, None])
    attn_probs = jax.nn.softmax(jnp.where(allowed, scores, -1e30), axis=-1).astype(jnp.bfloat16)
    return jnp.dot(attn_probs, values, preferred_element_type=jnp.float32).astype(jnp.bfloat16)


def layer_forward(x_in, ln_gain, w_qkv, w_out, w_up, w_down, seg_ids):
    rows = x_in.shape[0]
    x_f32 = x_in.astype(jnp.float32)
    normed = layer_norm(x_f32, ln_gain)
    flat = normed.reshape(rows * SEQ_LEN, HIDDEN)
    qkv_proj = jnp.dot(flat, w_qkv.reshape(HIDDEN, NUM_HEADS * 3 * HEAD_DIM), preferred_element_type=jnp.float32).astype(jnp.bfloat16)
    qkv_heads = qkv_proj.reshape(rows, SEQ_LEN, NUM_HEADS, 3, HEAD_DIM).transpose(0, 2, 3, 1, 4).reshape(rows * NUM_HEADS, 3, SEQ_LEN, HEAD_DIM)
    seg_rep = jnp.repeat(seg_ids, NUM_HEADS, axis=0)
    attn_out = lax.map(jax.checkpoint(head_attention), (qkv_heads, seg_rep))
    attn_flat = attn_out.reshape(rows, NUM_HEADS, SEQ_LEN, HEAD_DIM).transpose(0, 2, 1, 3).reshape(rows * SEQ_LEN, NUM_HEADS * HEAD_DIM)
    up_proj = jnp.dot(flat, w_up, preferred_element_type=jnp.float32).astype(jnp.bfloat16)
    hidden_act = jax.nn.gelu(up_proj.astype(jnp.float32), approximate=False).astype(jnp.bfloat16)
    share_sum = jnp.dot(attn_flat, w_out.reshape(NUM_HEADS * HEAD_DIM, HIDDEN), preferred_element_type=jnp.float32) + jnp.dot(hidden_act, w_down, preferred_element_type=jnp.float32)
    mixed = share_sum.astype(jnp.bfloat16).reshape(rows, SEQ_LEN, HIDDEN)
    return (x_f32 + mixed.astype(jnp.float32)).astype(jnp.bfloat16)


def reference(x_in, seg_ids, ln_gain, w_qkv, w_out, w_up, w_down, dy_in):
    def forward_fn(x_val, gain_val, qkv_val, out_val, up_val, down_val):
        return layer_forward(x_val, gain_val, qkv_val, out_val, up_val, down_val, seg_ids)
    y_out, vjp_fn = jax.vjp(forward_fn, x_in, ln_gain, w_qkv, w_out, w_up, w_down)
    dx_out, d_gain, d_wqkv, d_wout, d_wup, d_wdown = vjp_fn(dy_in)
    return (y_out, dx_out, d_gain, d_wqkv, d_wout, d_wup, d_wdown)
```

```python
import jax
import jax.numpy as jnp
from jax import lax
from jax.experimental import pallas as pl
from jax.experimental.pallas import tpu as pltpu

F32, BF16 = jnp.float32, jnp.bfloat16
MIB = 1 << 20
LN_EPS = 1e-5
NN = (((1,), (0,)), ((), ()))
NT = (((1,), (1,)), ((), ()))
TN = (((0,), (0,)), ((), ()))

def dot(x, w, dims=NN):
    return lax.dot_general(x, w, dims, preferred_element_type=F32)

def params(vmem=60, **kw):
    return pltpu.CompilerParams(vmem_limit_bytes=vmem * MIB, **kw)

def cost(flops, nbytes=0):
    return pl.CostEstimate(flops=int(flops), bytes_accessed=int(nbytes), transcendentals=0)

def ln_kernel(x_ref, g_ref, a_ref):
    x = x_ref[...].astype(F32)
    mean = jnp.mean(x, axis=-1, keepdims=True)
    cen = x - mean
    inv = lax.rsqrt(jnp.mean(cen * cen, axis=-1, keepdims=True) + LN_EPS)
    a_ref[...] = ((cen * inv) * g_ref[...].astype(F32)).astype(BF16)

def layer_norm(x, gain, tm=256):
    m, d = x.shape
    return pl.pallas_call(ln_kernel, grid=(m // tm,), in_specs=[pl.BlockSpec((tm, d), lambda i: (i, 0)), pl.BlockSpec((1, d), lambda i: (0, 0))],
        out_specs=pl.BlockSpec((tm, d), lambda i: (i, 0)), out_shape=jax.ShapeDtypeStruct((m, d), BF16), compiler_params=params(), name="layer_norm",
        cost_estimate=cost(12e9))(x, gain.reshape(1, d))

def unpair_kernel(z_ref, w_ref, s_ref):
    bk = w_ref.shape[0]
    s_ref[...] = z_ref[...].astype(F32)
    for n in range(2):
        for j in range(3):
            for t in range(2):
                w_ref[:, (n * 3 + j) * 256 + t * 128:(n * 3 + j) * 256 + t * 128 + 128] = s_ref[pl.ds(j * 4 + t * 2 + n, bk, stride=12), :].astype(BF16)

def pair_view(w):
    k = w.shape[0]
    return w.reshape(k, 2, 3, 2, 128).transpose(0, 2, 3, 1, 4).reshape(k * 12, 128)

def unpair_view(z):
    k = z.shape[0] // 12
    return z.reshape(k, 3, 2, 2, 128).transpose(0, 3, 1, 2, 4).reshape(k, 2, 3, 256)

def unpair(z, bk=256):
    k = z.shape[0] // 12
    return pl.pallas_call(unpair_kernel, grid=(k // bk,), in_specs=[pl.BlockSpec((bk * 12, 128), lambda i: (i, 0))],
        out_specs=pl.BlockSpec((bk, 1536), lambda i: (i, 0)), out_shape=jax.ShapeDtypeStruct((k, 1536), BF16), cost_estimate=cost(9e9),
        scratch_shapes=[pltpu.VMEM((bk * 12, 128), F32)], compiler_params=params(), name="unpair")(z)

def mm_kernel(x_ref, w_ref, o_ref):
    x = x_ref[...]
    o_ref[...] = dot(x, w_ref[...]).astype(o_ref.dtype)

def matmul(x, w, tm, tn):
    m, k = x.shape
    n = w.shape[1]
    return pl.pallas_call(mm_kernel, grid=(m // tm, n // tn), in_specs=[pl.BlockSpec((tm, k), lambda i, j: (i, 0)), pl.BlockSpec((k, tn), lambda i, j: (0, j))],
        out_specs=pl.BlockSpec((tm, tn), lambda i, j: (i, j)), out_shape=jax.ShapeDtypeStruct((m, n), BF16), compiler_params=params(), cost_estimate=cost(2 * m * n * k))(x, w)

def matmul_nt(x, w, tm, tn):
    m, k = x.shape
    n = w.shape[0]
    def body(x_ref, w_ref, o_ref):
        o_ref[...] = dot(x_ref[...], w_ref[...], NT).astype(o_ref.dtype)
    return pl.pallas_call(body, grid=(m // tm, n // tn), in_specs=[pl.BlockSpec((tm, k), lambda i, j: (i, 0)), pl.BlockSpec((tn, k), lambda i, j: (j, 0))],
        out_specs=pl.BlockSpec((tm, tn), lambda i, j: (i, j)), out_shape=jax.ShapeDtypeStruct((m, n), BF16), compiler_params=params(), cost_estimate=cost(2 * m * n * k))(x, w)

SQRT_HALF = 0.7071067811865476
INV_SQRT_2PI = 0.3989422804014327

def up_kernel(a_ref, w_ref, *refs):
    u_ref, h_ref = refs[-2:]
    u = dot(a_ref[...].reshape(-1, a_ref.shape[-1]), w_ref[...]).astype(BF16)
    u_ref[...] = u.reshape(u_ref.shape)
    uf = u.astype(F32)
    h_ref[...] = (0.5 * uf * (1.0 + lax.erf(uf * SQRT_HALF))).astype(BF16).reshape(h_ref.shape)

def up(a3, w, half, tb, tn, into=()):
    b, s, d = a3.shape
    n = w.shape[1]
    hs = s // 2
    spec = pl.BlockSpec((tb, hs, tn), lambda i, j: (i, half, j))
    return pl.pallas_call(up_kernel, grid=(b // tb, n // tn), in_specs=[pl.BlockSpec((tb, hs, d), lambda i, j: (i, half, 0)), pl.BlockSpec((d, tn), lambda i, j: (0, j))]
        + [pl.BlockSpec(memory_space=pl.ANY)] * len(into), input_output_aliases={2 + i: i for i in range(len(into))},
        out_specs=[spec, spec], out_shape=[jax.ShapeDtypeStruct((b, s, n), BF16)] * 2, compiler_params=params(), name="up",
        cost_estimate=cost(2 * b * hs * n * d))(a3, w, *into)

def dh_kernel(dy_ref, w_ref, u_ref, du_ref):
    dh = dot(dy_ref[...], w_ref[...], NT).astype(BF16).astype(F32)
    u = u_ref[...].astype(F32)
    grad = 0.5 * (1.0 + lax.erf(u * SQRT_HALF)) + u * (jnp.exp(-0.5 * (u * u)) * INV_SQRT_2PI)
    du_ref[...] = (dh * grad).astype(BF16)

def d_hidden(dy, w, u, tm, tn):
    m, d = dy.shape
    n = w.shape[0]
    spec = pl.BlockSpec((tm, tn), lambda i, j: (i, j))
    return pl.pallas_call(dh_kernel, grid=(m // tm, n // tn), in_specs=[pl.BlockSpec((tm, d), lambda i, j: (i, 0)), pl.BlockSpec((tn, d), lambda i, j: (j, 0)), spec],
        out_specs=spec, out_shape=jax.ShapeDtypeStruct((m, n), BF16), compiler_params=params(), name="d_hidden", cost_estimate=cost(2 * m * n * d))(dy, w, u)

def share_kernel(o_ref, h_ref, wo_ref, w2_ref, out_ref):
    f = lambda r: r[...].reshape(-1, r.shape[-1])
    out_ref[...] = (dot(f(o_ref), wo_ref[...]) + dot(f(h_ref), w2_ref[...])).astype(BF16).reshape(out_ref.shape)

def share_half(o3, h3, wo, w2, half, tb, tn):
    b, s, ko = o3.shape
    kh = h3.shape[2]
    n = wo.shape[1]
    hs = s // 2
    return pl.pallas_call(share_kernel, grid=(b // tb, n // tn), in_specs=[
        pl.BlockSpec((tb, hs, ko), lambda i, j: (i, half, 0)), pl.BlockSpec((tb, hs, kh), lambda i, j: (i, half, 0)),
        pl.BlockSpec((ko, tn), lambda i, j: (0, j)), pl.BlockSpec((kh, tn), lambda i, j: (0, j))],
        out_specs=pl.BlockSpec((tb, hs, tn), lambda i, j: (i, 0, j)), out_shape=jax.ShapeDtypeStruct((b, hs, n), BF16),
        compiler_params=params(), name="share", cost_estimate=cost(2 * b * hs * n * (ko + kh)))(o3, h3, wo, w2)

def d_share_kernel(dq_ref, du_ref, wq_ref, w1_ref, out_ref):
    f = lambda r: r[...].reshape(-1, r.shape[-1])
    out_ref[...] = (dot(f(dq_ref), wq_ref[...], NT) + dot(f(du_ref), w1_ref[...], NT)).astype(BF16).reshape(out_ref.shape)

def d_share_half(dq3, du3, wq, w1, half, tb, tn):
    b, s, kq = dq3.shape
    ku = du3.shape[2]
    n = wq.shape[0]
    hs = s // 2
    return pl.pallas_call(d_share_kernel, grid=(b // tb, n // tn), in_specs=[
        pl.BlockSpec((tb, hs, kq), lambda i, j: (i, half, 0)), pl.BlockSpec((tb, hs, ku), lambda i, j: (i, half, 0)),
        pl.BlockSpec((tn, kq), lambda i, j: (j, 0)), pl.BlockSpec((tn, ku), lambda i, j: (j, 0))],
        out_specs=pl.BlockSpec((tb, hs, tn), lambda i, j: (i, 0, j)), out_shape=jax.ShapeDtypeStruct((b, hs, n), BF16),
        compiler_params=params(), name="d_share", cost_estimate=cost(2 * b * hs * n * (kq + ku)))(dq3, du3, wq, w1)

def wgrad(x, g, tm, tn):
    k, m = x.shape
    n = g.shape[1]
    def body(x_ref, g_ref, o_ref):
        o_ref[...] = dot(x_ref[...], g_ref[...], TN).astype(BF16)
    return pl.pallas_call(body, grid=(m // tm, n // tn), in_specs=[pl.BlockSpec((k, tm), lambda i, j: (0, i)), pl.BlockSpec((k, tn), lambda i, j: (0, j))],
        out_specs=pl.BlockSpec((tm, tn), lambda i, j: (i, j)), out_shape=jax.ShapeDtypeStruct((m, n), BF16), compiler_params=params(), cost_estimate=cost(2 * m * n * k))(x, g)

def wgrad_qkv_kernel(a_ref, g_ref, z_ref, s_ref):
    bk = a_ref.shape[1]
    r = dot(a_ref[...], g_ref[...], TN)
    for n in range(2):
        for j in range(3):
            for t in range(2):
                c = (n * 3 + j) * 256 + t * 128
                s_ref[pl.ds(j * 4 + t * 2 + n, bk, stride=12), :] = r[:, c:c + 128]
    z_ref[...] = s_ref[...].astype(BF16)

def wgrad_qkv(a, g, bk=512):
    t, d = a.shape
    return pl.pallas_call(wgrad_qkv_kernel, grid=(d // bk,), in_specs=[pl.BlockSpec((t, bk), lambda i: (0, i)), pl.BlockSpec((t, 1536), lambda i: (0, 0))],
        out_specs=pl.BlockSpec((bk * 12, 128), lambda i: (i, 0)), out_shape=jax.ShapeDtypeStruct((d * 12, 128), BF16),
        scratch_shapes=[pltpu.VMEM((bk * 12, 128), F32)], compiler_params=params(), name="wgrad_qkv", cost_estimate=cost(2 * t * d * 1536))(a, g)

def att_probs(q, k, seg_c, seg_r):
    s = q.shape[0]
    sc = dot(q, k, NT) * (q.shape[1] ** -0.5)
    ok = (lax.broadcasted_iota(jnp.int32, (s, s), 1) <= lax.broadcasted_iota(jnp.int32, (s, s), 0)) & (seg_c == seg_r)
    sc = jnp.where(ok, sc, -1e30)
    e = jnp.exp(sc - jnp.max(sc, axis=-1, keepdims=True))
    return e / jnp.sum(e, axis=-1, keepdims=True)

def att_fwd_kernel(x_ref, segc_ref, segr_ref, o_ref):
    for n in range(2):
        q, k, v = (x_ref[0, :, (n * 3 + j) * 256:(n * 3 + j) * 256 + 256] for j in range(3))
        p = att_probs(q, k, segc_ref[0], segr_ref[0]).astype(BF16)
        o_ref[0, :, n * 256:n * 256 + 256] = dot(p, v).astype(BF16)

def att_fwd(qkv3, seg):
    b, s, c = qkv3.shape
    return pl.pallas_call(att_fwd_kernel, grid=(b,), in_specs=[pl.BlockSpec((1, s, c), lambda i: (i, 0, 0)),
        pl.BlockSpec((1, s, 1), lambda i: (i, 0, 0)), pl.BlockSpec((1, 1, s), lambda i: (i, 0, 0))],
        out_specs=pl.BlockSpec((1, s, 512), lambda i: (i, 0, 0)), out_shape=jax.ShapeDtypeStruct((b, s, 512), BF16),
        compiler_params=params(), name="att_fwd", cost_estimate=cost(8e9))(qkv3, seg[:, :, None], seg[:, None, :])

def att_bwd_kernel(x_ref, do_ref, segc_ref, segr_ref, dx_ref):
    for n in range(2):
        c = n * 768
        q, k, v = (x_ref[0, :, c + j * 256:c + j * 256 + 256] for j in range(3))
        do = do_ref[0, :, n * 256:n * 256 + 256]
        p = att_probs(q, k, segc_ref[0], segr_ref[0])
        dp = dot(do, v, NT)
        ds = (p * (dp - jnp.sum(dp * p, axis=-1, keepdims=True)) * (256 ** -0.5)).astype(BF16)
        dx_ref[0, :, c:c + 256] = dot(ds, k).astype(BF16)
        dx_ref[0, :, c + 256:c + 512] = dot(ds, q, TN).astype(BF16)
        dx_ref[0, :, c + 512:c + 768] = dot(p.astype(BF16), do, TN).astype(BF16)

def att_bwd(qkv3, do3, seg):
    b, s, c = qkv3.shape
    return pl.pallas_call(att_bwd_kernel, grid=(b,), in_specs=[pl.BlockSpec((1, s, c), lambda i: (i, 0, 0)), pl.BlockSpec((1, s, 512), lambda i: (i, 0, 0)),
        pl.BlockSpec((1, s, 1), lambda i: (i, 0, 0)), pl.BlockSpec((1, 1, s), lambda i: (i, 0, 0))],
        out_specs=pl.BlockSpec((1, s, c), lambda i: (i, 0, 0)), out_shape=jax.ShapeDtypeStruct((b, s, c), BF16),
        compiler_params=params(), name="att_bwd", cost_estimate=cost(12e9))(qkv3, do3, seg[:, :, None], seg[:, None, :])
from jax.sharding import PartitionSpec as P


def after(x, *deps):
    return lax.optimization_barrier((x, *deps))[0]


def solution(mesh):
    def body(x_in, seg_ids, ln_gain, w_qkv, w_out, w_up, w_down, dy_in):
        rows, seq, hid = x_in.shape
        tok = rows * seq
        me = lax.axis_index('model')
        x2, dy2 = x_in.reshape(tok, hid), dy_in.reshape(tok, hid)
        three = lambda v: v.reshape(rows, seq, -1)
        wo = w_out.reshape(-1, hid)
        normed = layer_norm(x2, ln_gain, tm=512)
        wq = unpair(pair_view(w_qkv), bk=512)
        qkv = matmul(normed, wq, 1024, 512)
        attn = att_fwd(three(qkv), seg_ids)
        scatter = lambda v: lax.psum_scatter(v, 'model', scatter_dimension=0, tiled=True)
        u_a, h_a = up(three(normed), w_up, 0, 8, 512)
        share_a = share_half(attn, h_a, wo, w_down, 0, 8, 512)
        m_a = scatter(share_a)
        u, h = up(after(three(normed), share_a), w_up, 1, 8, 512, (u_a, h_a))
        share_b = share_half(attn, h, wo, w_down, 1, 8, 512)
        m_b = scatter(share_b)
        dy_l = after(dy2, share_b)
        d_attn = matmul_nt(dy_l, wo, 512, 512)
        d_qkv = att_bwd(three(qkv), three(d_attn), seg_ids)
        u, h = u.reshape(tok, -1), h.reshape(tok, -1)
        d_up = d_hidden(dy_l, w_down, u, 1024, 512)
        x_own = lax.dynamic_slice_in_dim(x_in, me, 1, 0).astype(F32)
        mixed = after(jnp.concatenate([m_a, m_b], axis=1), d_up, d_qkv)
        y_own = (x_own + mixed.astype(F32)).astype(BF16)
        y_out = lax.all_gather(y_own, 'model', axis=0, tiled=True)
        ds_a = d_share_half(after(d_qkv, y_own), three(d_up), wq, w_up, 0, 8, 512)
        dn_a = scatter(ds_a)
        ds_b = d_share_half(after(d_qkv, ds_a), three(d_up), wq, w_up, 1, 8, 512)
        dn_b = scatter(ds_b)
        dy_own = lax.dynamic_slice_in_dim(dy_in, me, 1, 0).astype(F32)
        mean = jnp.mean(x_own, axis=-1, keepdims=True)
        cen = x_own - mean
        inv = lax.rsqrt(jnp.mean(cen * cen, axis=-1, keepdims=True) + LN_EPS)
        nf = cen * inv
        grad = jnp.concatenate([dn_a, dn_b], axis=1).astype(F32)
        dg_part = jnp.sum(grad * nf, axis=(0, 1))
        d_hat = grad * ln_gain.astype(F32)
        d_x = inv * (d_hat - jnp.mean(d_hat, axis=-1, keepdims=True) - nf * jnp.mean(d_hat * nf, axis=-1, keepdims=True))
        dx_own = (dy_own + d_x).astype(BF16)
        dx_out = lax.all_gather(dx_own, 'model', axis=0, tiled=True)
        d_gain = lax.psum(dg_part, 'model').astype(BF16)
        late = lambda v: after(v, ds_b)
        a_l, dy_w = late(normed), late(dy2)
        d_wdown = wgrad(h, dy_w, 1024, 1024)
        d_wup = wgrad(a_l, d_up, 1024, 1024)
        d_wqkv = unpair_view(wgrad_qkv(a_l, d_qkv.reshape(tok, -1)))
        d_wout = wgrad(attn.reshape(tok, -1), dy_w, 512, 1024).reshape(w_out.shape)
        return y_out, dx_out, d_gain, d_wqkv, d_wout, d_wup, d_wdown

    in_specs = (P('data'), P('data'), P(), P(None, 'model'), P('model'), P(None, 'model'), P('model'), P('data'))
    out_specs = (P('data'), P('data'), P('data'), P('data', 'model'), P(('data', 'model')), P('data', 'model'), P(('data', 'model')))
    return jax.shard_map(body, mesh=mesh, in_specs=in_specs, out_specs=out_specs, check_vma=False)
```

```python
import jax
import jax.numpy as jnp
from jax import lax
from jax.experimental import pallas as pl
from jax.experimental.pallas import tpu as pltpu

F32, BF16 = jnp.float32, jnp.bfloat16
MIB = 1 << 20
LN_EPS = 1e-5
NN = (((1,), (0,)), ((), ()))
NT = (((1,), (1,)), ((), ()))
TN = (((0,), (0,)), ((), ()))

def dot(x, w, dims=NN):
    return lax.dot_general(x, w, dims, preferred_element_type=F32)

def params(vmem=60, **kw):
    return pltpu.CompilerParams(vmem_limit_bytes=vmem * MIB, **kw)

def cost(flops, nbytes=0):
    return pl.CostEstimate(flops=int(flops), bytes_accessed=int(nbytes), transcendentals=0)

def ln_kernel(x_ref, g_ref, a_ref):
    x = x_ref[...].astype(F32)
    mean = jnp.mean(x, axis=-1, keepdims=True)
    cen = x - mean
    inv = lax.rsqrt(jnp.mean(cen * cen, axis=-1, keepdims=True) + LN_EPS)
    a_ref[...] = ((cen * inv) * g_ref[...].astype(F32)).astype(BF16)

def layer_norm(x, gain, tm=256):
    m, d = x.shape
    return pl.pallas_call(ln_kernel, grid=(m // tm,), in_specs=[pl.BlockSpec((tm, d), lambda i: (i, 0)), pl.BlockSpec((1, d), lambda i: (0, 0))],
        out_specs=pl.BlockSpec((tm, d), lambda i: (i, 0)), out_shape=jax.ShapeDtypeStruct((m, d), BF16), compiler_params=params(), name="layer_norm",
        cost_estimate=cost(12e9))(x, gain.reshape(1, d))

def unpair_kernel(z_ref, w_ref, s_ref):
    bk = w_ref.shape[0]
    s_ref[...] = z_ref[...].astype(F32)
    for n in range(2):
        for j in range(3):
            for t in range(2):
                w_ref[:, (n * 3 + j) * 256 + t * 128:(n * 3 + j) * 256 + t * 128 + 128] = s_ref[pl.ds(j * 4 + t * 2 + n, bk, stride=12), :].astype(BF16)

def pair_view(w):
    k = w.shape[0]
    return w.reshape(k, 2, 3, 2, 128).transpose(0, 2, 3, 1, 4).reshape(k * 12, 128)

def unpair_view(z):
    k = z.shape[0] // 12
    return z.reshape(k, 3, 2, 2, 128).transpose(0, 3, 1, 2, 4).reshape(k, 2, 3, 256)

def unpair(z, bk=256):
    k = z.shape[0] // 12
    return pl.pallas_call(unpair_kernel, grid=(k // bk,), in_specs=[pl.BlockSpec((bk * 12, 128), lambda i: (i, 0))],
        out_specs=pl.BlockSpec((bk, 1536), lambda i: (i, 0)), out_shape=jax.ShapeDtypeStruct((k, 1536), BF16), cost_estimate=cost(9e9),
        scratch_shapes=[pltpu.VMEM((bk * 12, 128), F32)], compiler_params=params(), name="unpair")(z)

def mm_kernel(x_ref, w_ref, o_ref):
    x = x_ref[...]
    o_ref[...] = dot(x, w_ref[...]).astype(o_ref.dtype)

def matmul(x, w, tm, tn):
    m, k = x.shape
    n = w.shape[1]
    return pl.pallas_call(mm_kernel, grid=(m // tm, n // tn), in_specs=[pl.BlockSpec((tm, k), lambda i, j: (i, 0)), pl.BlockSpec((k, tn), lambda i, j: (0, j))],
        out_specs=pl.BlockSpec((tm, tn), lambda i, j: (i, j)), out_shape=jax.ShapeDtypeStruct((m, n), BF16), compiler_params=params(), cost_estimate=cost(2 * m * n * k))(x, w)

def matmul_nt(x, w, tm, tn):
    m, k = x.shape
    n = w.shape[0]

    def body(x_ref, w_ref, o_ref):
        o_ref[...] = dot(x_ref[...], w_ref[...], NT).astype(o_ref.dtype)

    return pl.pallas_call(body, grid=(m // tm, n // tn), in_specs=[pl.BlockSpec((tm, k), lambda i, j: (i, 0)), pl.BlockSpec((tn, k), lambda i, j: (j, 0))],
        out_specs=pl.BlockSpec((tm, tn), lambda i, j: (i, j)), out_shape=jax.ShapeDtypeStruct((m, n), BF16), compiler_params=params(), cost_estimate=cost(2 * m * n * k))(x, w)

SQRT_HALF = 0.7071067811865476
INV_SQRT_2PI = 0.3989422804014327

def up_kernel(a_ref, w_ref, u_ref, h_ref):
    u = dot(a_ref[...].reshape(-1, a_ref.shape[-1]), w_ref[...]).astype(BF16)
    u_ref[...] = u.reshape(u_ref.shape)
    uf = u.astype(F32)
    h_ref[...] = (0.5 * uf * (1.0 + lax.erf(uf * SQRT_HALF))).astype(BF16).reshape(h_ref.shape)

def up(a3, w, half, tb, tn):
    b, s, d = a3.shape
    n = w.shape[1]
    hs = s // 2
    spec = pl.BlockSpec((tb, hs, tn), lambda i, j: (i, 0, j))
    return pl.pallas_call(up_kernel, grid=(b // tb, n // tn), in_specs=[pl.BlockSpec((tb, hs, d), lambda i, j: (i, half, 0)), pl.BlockSpec((d, tn), lambda i, j: (0, j))],
        out_specs=[spec, spec], out_shape=[jax.ShapeDtypeStruct((b, hs, n), BF16)] * 2, compiler_params=params(), name="up",
        cost_estimate=cost(2 * b * hs * n * d))(a3, w)

def gelu_grad(dy, w, u):
    dh = dot(dy, w, NT).astype(BF16).astype(F32)
    u = u.astype(F32)
    grad = 0.5 * (1.0 + lax.erf(u * SQRT_HALF)) + u * (jnp.exp(-0.5 * (u * u)) * INV_SQRT_2PI)
    return (dh * grad).astype(BF16)

def wgrad(x, g, tm, tn):
    k, m = x.shape
    n = g.shape[1]

    def body(x_ref, g_ref, o_ref):
        o_ref[...] = dot(x_ref[...], g_ref[...], TN).astype(BF16)

    return pl.pallas_call(body, grid=(m // tm, n // tn), in_specs=[pl.BlockSpec((k, tm), lambda i, j: (0, i)), pl.BlockSpec((k, tn), lambda i, j: (0, j))],
        out_specs=pl.BlockSpec((tm, tn), lambda i, j: (i, j)), out_shape=jax.ShapeDtypeStruct((m, n), BF16), compiler_params=params(), cost_estimate=cost(2 * m * n * k))(x, g)

def wgrad_qkv_kernel(a_ref, g_ref, z_ref, s_ref):
    bk = a_ref.shape[1]
    r = dot(a_ref[...], g_ref[...], TN)
    for n in range(2):
        for j in range(3):
            for t in range(2):
                c = (n * 3 + j) * 256 + t * 128
                s_ref[pl.ds(j * 4 + t * 2 + n, bk, stride=12), :] = r[:, c:c + 128]
    z_ref[...] = s_ref[...].astype(BF16)

def wgrad_qkv(a, g, bk=512):
    t, d = a.shape
    return pl.pallas_call(wgrad_qkv_kernel, grid=(d // bk,), in_specs=[pl.BlockSpec((t, bk), lambda i: (0, i)), pl.BlockSpec((t, 1536), lambda i: (0, 0))],
        out_specs=pl.BlockSpec((bk * 12, 128), lambda i: (i, 0)), out_shape=jax.ShapeDtypeStruct((d * 12, 128), BF16),
        scratch_shapes=[pltpu.VMEM((bk * 12, 128), F32)], compiler_params=params(), name="wgrad_qkv", cost_estimate=cost(2 * t * d * 1536))(a, g)

def att_probs(q, k, seg_c, seg_r):
    s = q.shape[0]
    sc = dot(q, k, NT) * (q.shape[1] ** -0.5)
    ok = (lax.broadcasted_iota(jnp.int32, (s, s), 1) <= lax.broadcasted_iota(jnp.int32, (s, s), 0)) & (seg_c == seg_r)
    sc = jnp.where(ok, sc, -1e30)
    e = jnp.exp(sc - jnp.max(sc, axis=-1, keepdims=True))
    return e / jnp.sum(e, axis=-1, keepdims=True)

def att_fwd_kernel(x_ref, segc_ref, segr_ref, o_ref):
    for n in range(2):
        q, k, v = (x_ref[0, :, (n * 3 + j) * 256:(n * 3 + j) * 256 + 256] for j in range(3))
        p = att_probs(q, k, segc_ref[0], segr_ref[0]).astype(BF16)
        o_ref[0, :, n * 256:n * 256 + 256] = dot(p, v).astype(BF16)

def att_fwd(qkv3, seg):
    b, s, c = qkv3.shape
    return pl.pallas_call(att_fwd_kernel, grid=(b,), in_specs=[pl.BlockSpec((1, s, c), lambda i: (i, 0, 0)),
        pl.BlockSpec((1, s, 1), lambda i: (i, 0, 0)), pl.BlockSpec((1, 1, s), lambda i: (i, 0, 0))],
        out_specs=pl.BlockSpec((1, s, 512), lambda i: (i, 0, 0)), out_shape=jax.ShapeDtypeStruct((b, s, 512), BF16),
        compiler_params=params(), name="att_fwd", cost_estimate=cost(8e9))(qkv3, seg[:, :, None], seg[:, None, :])

def att_bwd_kernel(x_ref, do_ref, segc_ref, segr_ref, dx_ref):
    for n in range(2):
        c = n * 768
        q, k, v = (x_ref[0, :, c + j * 256:c + j * 256 + 256] for j in range(3))
        do = do_ref[0, :, n * 256:n * 256 + 256]
        p = att_probs(q, k, segc_ref[0], segr_ref[0])
        dp = dot(do, v, NT)
        ds = (p * (dp - jnp.sum(dp * p, axis=-1, keepdims=True)) * (256 ** -0.5)).astype(BF16)
        dx_ref[0, :, c:c + 256] = dot(ds, k).astype(BF16)
        dx_ref[0, :, c + 256:c + 512] = dot(ds, q, TN).astype(BF16)
        dx_ref[0, :, c + 512:c + 768] = dot(p.astype(BF16), do, TN).astype(BF16)

def att_bwd(qkv3, do3, seg):
    b, s, c = qkv3.shape
    return pl.pallas_call(att_bwd_kernel, grid=(b,), in_specs=[pl.BlockSpec((1, s, c), lambda i: (i, 0, 0)), pl.BlockSpec((1, s, 512), lambda i: (i, 0, 0)),
        pl.BlockSpec((1, s, 1), lambda i: (i, 0, 0)), pl.BlockSpec((1, 1, s), lambda i: (i, 0, 0))],
        out_specs=pl.BlockSpec((1, s, c), lambda i: (i, 0, 0)), out_shape=jax.ShapeDtypeStruct((b, s, c), BF16),
        compiler_params=params(), name="att_bwd", cost_estimate=cost(12e9))(qkv3, do3, seg[:, :, None], seg[:, None, :])


MESH = pl.DeviceIdType.MESH


def rem(a, b):
    return lax.rem(a, jnp.int32(b))


def product_scatter(cid, lhs, rhs, dims, hs, tn, steps2, in2, specs2, outs2, ospecs2, body2, flops, LAG=3):
    chips = lhs[0][0].shape[0] // 2
    hid = rhs[0].shape[1 - dims[0][1][0]]
    t1 = hid // tn
    total = t1 + steps2
    assert steps2 > LAG
    nl, n2, no2 = len(lhs), len(in2), len(outs2)
    halves = [half for _, half in lhs]
    lhs = [v.reshape(chips, 2, *v.shape[1:]) for v, _ in lhs]
    early = lambda i: jnp.minimum(i, t1 - 1)
    late = lambda i: jnp.maximum(i - t1, 0)
    once = dict(pipeline_mode=pl.Buffered(1))
    in_specs = [pl.BlockSpec((chips, 2, hs, v.shape[3]), lambda i, half=half: (0, 0, half, 0), **once) for v, half in zip(lhs, halves)]
    if dims is NN:
        in_specs += [pl.BlockSpec((w.shape[0], tn), lambda i: (0, early(i))) for w in rhs]
    else:
        in_specs += [pl.BlockSpec((tn, w.shape[1]), lambda i: (early(i), 0)) for w in rhs]
    shift = lambda sp: sp if sp.index_map is None else pl.BlockSpec(sp.block_shape, lambda i, m=sp.index_map: m(late(i)), pipeline_mode=sp.pipeline_mode)
    in_specs += [shift(sp) for sp in specs2]
    anyspec = pl.BlockSpec(memory_space=pl.ANY)
    out_specs = [anyspec] * 3 + [shift(sp) for sp in ospecs2]
    part = jax.ShapeDtypeStruct((hs, hid), BF16)

    def kernel(*refs):
        lrefs, wrefs, refs = refs[:nl], refs[nl:2 * nl], refs[2 * nl:]
        in2_refs, refs = refs[:n2], refs[n2:]
        own_ref, left_ref, right_ref = refs[:3]
        out2_refs, refs = refs[3:3 + no2], refs[3 + no2:]
        pair_out, pair_in, acc, fwd, s_pair, r_pair, s_far, r_far, s_left, s_right, r_left, r_right, s_own = refs
        i = pl.program_id(0)
        me = lax.axis_index('model')
        core = rem(me, 2)
        chip = lax.div(me, jnp.int32(2))
        c_right, c_left, c_far = rem(chip + 1, chips), rem(chip + chips - 1, chips), rem(chip + 2, chips)
        partner, to_right, to_left = me + 1 - 2 * core, c_right * 2 + core, c_left * 2 + core

        def remote(src, dst, ss, rs, dev):
            return pltpu.make_async_remote_copy(src_ref=src, dst_ref=dst, send_sem=ss, recv_sem=rs, device_id={'model': dev}, device_id_type=MESH)

        cols = lambda ref, k: ref.at[:, pl.ds(pl.multiple_of(k * tn, tn), tn)]
        pair = lambda k: remote(pair_out.at[rem(k, 2)], pair_in.at[k], s_pair.at[rem(k, 2)], r_pair.at[k], partner)
        far = lambda k, dev: remote(acc.at[k, c_far], fwd.at[k], s_far.at[k], r_far.at[k], dev)
        leftward = lambda k: remote(acc.at[k, c_left], cols(right_ref, k), s_left.at[k], r_right.at[k], to_left)
        rightward = lambda k: remote(acc.at[k, c_right], cols(left_ref, k), s_right.at[k], r_left.at[k], to_right)
        keep = lambda k: pltpu.make_async_copy(acc.at[k, chip], cols(own_ref, k), s_own.at[k])

        @pl.when(i == 0)
        def _():
            barrier = pltpu.get_barrier_semaphore()
            for dev in (partner, to_left, to_right):
                pl.semaphore_signal(barrier, inc=1, device_id={'model': dev}, device_id_type=MESH)
            pl.semaphore_wait(barrier, 3)

        @pl.when((i >= 1) & (i <= t1))
        def _():
            k = i - 1
            pair(k).wait_recv()
            acc[k] = (acc[k].astype(F32) + pair_in[k].astype(F32)).astype(BF16)
            keep(k).start()

            @pl.when(rem(k, 2) == 0)
            def _():
                far(k, to_right).start()
                leftward(k).start()

            @pl.when(rem(k, 2) == 1)
            def _():
                far(k, to_left).start()
                rightward(k).start()

        @pl.when((i >= 1 + LAG) & (i <= t1 + LAG))
        def _():
            k = i - 1 - LAG
            far(k, to_right).wait_recv()

            @pl.when(rem(k, 2) == 0)
            def _():
                acc[k, c_right] = (acc[k, c_right].astype(F32) + fwd[k].astype(F32)).astype(BF16)
                rightward(k).start()

            @pl.when(rem(k, 2) == 1)
            def _():
                acc[k, c_left] = (acc[k, c_left].astype(F32) + fwd[k].astype(F32)).astype(BF16)
                leftward(k).start()

        @pl.when(i < t1)
        def _():
            def tile(p):
                r = None
                for x, w in zip(lrefs, wrefs):
                    v = dot(x[:, p].reshape(chips * hs, x.shape[3]), w[...], dims)
                    r = v if r is None else r + v
                return r.astype(BF16).reshape(chips, hs, tn)

            @pl.when(i >= 2)
            def _():
                pair(i - 2).wait_send()

            pair_out[rem(i, 2)] = tile(1 - core)
            pair(i).start()
            acc[i] = tile(core)

        @pl.when(i >= t1)
        def _():
            body2(i - t1, *in2_refs, *out2_refs)

        @pl.when(i == total - 1)
        def _():
            for k in range(t1 - 2, t1):
                pair(jnp.int32(k)).wait_send()

            def drain(k, carry):
                far(k, to_right).wait_send()
                leftward(k).wait_send()
                rightward(k).wait_send()
                keep(k).wait()
                rightward(k).wait_recv()
                leftward(k).wait_recv()
                return carry

            lax.fori_loop(jnp.int32(0), jnp.int32(t1), drain, jnp.int32(0))

    dma = pltpu.SemaphoreType.DMA
    outs = pl.pallas_call(kernel, grid=(total,), in_specs=in_specs, out_specs=out_specs, out_shape=[part] * 3 + list(outs2),
        scratch_shapes=[pltpu.VMEM((2, chips, hs, tn), BF16), pltpu.VMEM((t1, chips, hs, tn), BF16), pltpu.VMEM((t1, chips, hs, tn), BF16), pltpu.VMEM((t1, hs, tn), BF16),
            dma((2,)), dma((t1,)), dma((t1,)), dma((t1,)), dma((t1,)), dma((t1,)), dma((t1,)), dma((t1,)), dma((t1,))],
        compiler_params=params(63, collective_id=cid, has_side_effects=True), cost_estimate=cost(flops))(*lhs, *rhs, *in2)
    return outs[:3], outs[3:]


def scatter_up(cid, attn, h_a, wo, w_down, a3, w_up, tn=512):
    b, s, d = a3.shape
    n, hs = w_up.shape[1], s // 2
    spec = pl.BlockSpec((b, hs, tn), lambda t: (0, 0, t))

    def body2(t, a_ref, w_ref, u_ref, h_ref):
        up_kernel(a_ref, w_ref, u_ref, h_ref)

    return product_scatter(cid, [(attn, 0), (h_a, 0)], [wo, w_down], NN, hs, tn, n // tn, [a3, w_up],
        [pl.BlockSpec((b, hs, d), lambda t: (0, 1, 0), pipeline_mode=pl.Buffered(1)), pl.BlockSpec((d, tn), lambda t: (0, t))],
        [jax.ShapeDtypeStruct((b, hs, n), BF16)] * 2, [spec, spec], body2, 4e10, 3)


def scatter_dh(cid, attn, h_b, wo, w_down, dy3, u_a, u_b, tn=512):
    b, s, d = dy3.shape
    n, hs = w_down.shape[0], s // 2
    nt = n // tn

    def body2(t, dy_ref, w_ref, ua_ref, ub_ref, du_ref):
        u = jnp.where(t < nt, ua_ref[...], ub_ref[...]).reshape(b * hs, tn)
        du_ref[...] = gelu_grad(dy_ref[...].reshape(b * hs, d), w_ref[...], u).reshape(b, hs, tn)

    return product_scatter(cid, [(attn, 1), (h_b, 0)], [wo, w_down], NN, hs, tn, 2 * nt, [dy3, w_down, u_a, u_b],
        [pl.BlockSpec((b, hs, d), lambda t: (0, t // nt, 0)), pl.BlockSpec((tn, d), lambda t: (t % nt, 0)),
         pl.BlockSpec((b, hs, tn), lambda t: (0, 0, jnp.minimum(t, nt - 1))), pl.BlockSpec((b, hs, tn), lambda t: (0, 0, jnp.maximum(t - nt, 0)))],
        [jax.ShapeDtypeStruct((b, s, n), BF16)], [pl.BlockSpec((b, hs, tn), lambda t: (0, t // nt, t % nt))], body2, 6e10, 6)


def scatter_wout(cid, half, d_qkv, d_up, wq, w_up, attn2, dy2, tn=512, tn2=512):
    t, d = dy2.shape
    k = attn2.shape[1]
    hs = d_qkv.shape[1] // 2

    def body2(i, x_ref, g_ref, o_ref):
        o_ref[...] = dot(x_ref[...], g_ref[...], TN).astype(BF16)

    return product_scatter(cid, [(d_qkv, half), (d_up, half)], [wq, w_up], NT, hs, tn, d // tn2, [attn2, dy2],
        [pl.BlockSpec((t, k), lambda i: (0, 0), pipeline_mode=pl.Buffered(1)), pl.BlockSpec((t, tn2), lambda i: (0, i))],
        [jax.ShapeDtypeStruct((k, d), BF16)], [pl.BlockSpec((k, tn2), lambda i: (0, i))], body2, 4e10, 3)


def scatter_wdown(cid, half, d_qkv, d_up, wq, w_up, h_a, h_b, dy3, tn=512, tm2=1024, tn2=1024):
    b, s, d = dy3.shape
    n, hs = h_a.shape[2], s // 2
    cols = d // tn2

    def body2(i, xa_ref, xb_ref, g_ref, o_ref):
        rows = lambda v: v.reshape(b * hs, v.shape[2])
        o_ref[...] = (dot(rows(xa_ref[...]), rows(g_ref[:, :hs]), TN) + dot(rows(xb_ref[...]), rows(g_ref[:, hs:]), TN)).astype(BF16)

    x_spec = pl.BlockSpec((b, hs, tm2), lambda i: (0, 0, i // cols))
    return product_scatter(cid, [(d_qkv, half), (d_up, half)], [wq, w_up], NT, hs, tn, (n // tm2) * cols, [h_a, h_b, dy3],
        [x_spec, x_spec, pl.BlockSpec((b, s, tn2), lambda i: (0, 0, i % cols))],
        [jax.ShapeDtypeStruct((n, d), BF16)], [pl.BlockSpec((tm2, tn2), lambda i: (i // cols, i % cols))], body2, 7e10, 5)
from jax.sharding import PartitionSpec as P


def after(x, *deps):
    return lax.optimization_barrier((x, *deps))[0]


def solution(mesh):
    def body(x_in, seg_ids, ln_gain, w_qkv, w_out, w_up, w_down, dy_in):
        rows, seq, hid = x_in.shape
        tok = rows * seq
        hs = seq // 2
        me = lax.axis_index('model')
        x2, dy2 = x_in.reshape(tok, hid), dy_in.reshape(tok, hid)
        three = lambda v: v.reshape(rows, seq, -1)
        wo = w_out.reshape(-1, hid)
        wq = unpair(pair_view(w_qkv), bk=512)
        normed = layer_norm(x2, ln_gain, tm=512)
        qkv = matmul(normed, wq, 1024, 512)
        attn = att_fwd(three(qkv), seg_ids)
        u_a, h_a = up(three(normed), w_up, 0, 8, 512)
        own = lambda v: lax.dynamic_slice_in_dim(v, me, 1, 0)
        total = lambda p: sum(v.astype(F32) for v in p).astype(BF16)
        gather = lambda v: lax.all_gather(v, 'model', axis=0, tiled=True)
        x_own = own(x_in).astype(F32)

        part_a, (u_b, h_b) = scatter_up(1, attn, h_a, wo, w_down, three(normed), w_up)
        y_a = (x_own[0, :hs] + total(part_a).astype(F32)).astype(BF16)
        y_a_all = gather(y_a[None])
        part_b, (d_up,) = scatter_dh(2, attn, h_b, wo, after(w_down, y_a), dy_in, u_a, u_b)
        y_b = (x_own[0, hs:] + total(part_b).astype(F32)).astype(BF16)
        y_b_all = gather(y_b[None])
        d_attn = matmul_nt(after(dy2, d_up, y_b), wo, 512, 512)
        d_qkv = att_bwd(three(qkv), three(d_attn), seg_ids)
        dn_a, (d_wout,) = scatter_wout(3, 0, after(d_qkv, y_b), d_up, wq, w_up, attn.reshape(tok, -1), dy2)
        dn_b, (d_wdown,) = scatter_wdown(4, 1, after(d_qkv, d_wout), d_up, wq, w_up, h_a, h_b, dy_in)

        dy_own = own(dy_in).astype(F32)
        mean = jnp.mean(x_own, axis=-1, keepdims=True)
        cen = x_own - mean
        inv = lax.rsqrt(jnp.mean(cen * cen, axis=-1, keepdims=True) + LN_EPS)
        nf = cen * inv
        grad = jnp.concatenate([total(dn_a), total(dn_b)], axis=0)[None].astype(F32)
        dg_part = jnp.sum(grad * nf, axis=(0, 1))
        d_hat = grad * ln_gain.astype(F32)
        d_x = inv * (d_hat - jnp.mean(d_hat, axis=-1, keepdims=True) - nf * jnp.mean(d_hat * nf, axis=-1, keepdims=True))
        dx_own = (dy_own + d_x).astype(BF16)
        dx_out = gather(dx_own)
        d_gain = lax.psum(dg_part, 'model').astype(BF16)
        a_l = after(normed, dx_own)
        d_wqkv = unpair_view(wgrad_qkv(a_l, d_qkv.reshape(tok, -1)))
        d_wup = wgrad(a_l, d_up.reshape(tok, -1), 1024, 1024)
        y_out = jnp.concatenate([y_a_all, y_b_all], axis=1)
        return y_out, dx_out, d_gain, d_wqkv, d_wout.reshape(w_out.shape), d_wup, d_wdown

    in_specs = (P('data'), P('data'), P(), P(None, 'model'), P('model'), P(None, 'model'), P('model'), P('data'))
    out_specs = (P('data'), P('data'), P('data'), P('data', 'model'), P(('data', 'model')), P('data', 'model'), P(('data', 'model')))
    return jax.shard_map(body, mesh=mesh, in_specs=in_specs, out_specs=out_specs, check_vma=False)
```

```python
import jax
import jax.numpy as jnp
from jax import lax
from jax.experimental import pallas as pl
from jax.experimental.pallas import tpu as pltpu

F32, BF16 = jnp.float32, jnp.bfloat16
MIB = 1 << 20
LN_EPS = 1e-5
NN = (((1,), (0,)), ((), ()))
NT = (((1,), (1,)), ((), ()))
TN = (((0,), (0,)), ((), ()))

def dot(x, w, dims=NN):
    return lax.dot_general(x, w, dims, preferred_element_type=F32)

def params(vmem=60, **kw):
    return pltpu.CompilerParams(vmem_limit_bytes=vmem * MIB, **kw)

def cost(flops, nbytes=0):
    return pl.CostEstimate(flops=int(flops), bytes_accessed=int(nbytes), transcendentals=0)

def ln_kernel(x_ref, g_ref, a_ref):
    x = x_ref[...].astype(F32)
    mean = jnp.mean(x, axis=-1, keepdims=True)
    cen = x - mean
    inv = lax.rsqrt(jnp.mean(cen * cen, axis=-1, keepdims=True) + LN_EPS)
    a_ref[...] = ((cen * inv) * g_ref[...].astype(F32)).astype(BF16)

def layer_norm(x, gain, tm=256):
    m, d = x.shape
    return pl.pallas_call(ln_kernel, grid=(m // tm,), in_specs=[pl.BlockSpec((tm, d), lambda i: (i, 0)), pl.BlockSpec((1, d), lambda i: (0, 0))],
        out_specs=pl.BlockSpec((tm, d), lambda i: (i, 0)), out_shape=jax.ShapeDtypeStruct((m, d), BF16), compiler_params=params(), name="layer_norm",
        cost_estimate=cost(12e9))(x, gain.reshape(1, d))

def unpair_kernel(z_ref, w_ref, s_ref):
    bk = w_ref.shape[0]
    s_ref[...] = z_ref[...].astype(F32)
    for n in range(2):
        for j in range(3):
            for t in range(2):
                w_ref[:, (n * 3 + j) * 256 + t * 128:(n * 3 + j) * 256 + t * 128 + 128] = s_ref[pl.ds(j * 4 + t * 2 + n, bk, stride=12), :].astype(BF16)

def pair_view(w):
    k = w.shape[0]
    return w.reshape(k, 2, 3, 2, 128).transpose(0, 2, 3, 1, 4).reshape(k * 12, 128)

def unpair_view(z):
    k = z.shape[0] // 12
    return z.reshape(k, 3, 2, 2, 128).transpose(0, 3, 1, 2, 4).reshape(k, 2, 3, 256)

def unpair(z, bk=256):
    k = z.shape[0] // 12
    return pl.pallas_call(unpair_kernel, grid=(k // bk,), in_specs=[pl.BlockSpec((bk * 12, 128), lambda i: (i, 0))],
        out_specs=pl.BlockSpec((bk, 1536), lambda i: (i, 0)), out_shape=jax.ShapeDtypeStruct((k, 1536), BF16), cost_estimate=cost(9e9),
        scratch_shapes=[pltpu.VMEM((bk * 12, 128), F32)], compiler_params=params(), name="unpair")(z)

def mm_kernel(x_ref, w_ref, o_ref):
    x = x_ref[...]
    o_ref[...] = dot(x, w_ref[...]).astype(o_ref.dtype)

def matmul(x, w, tm, tn):
    m, k = x.shape
    n = w.shape[1]
    return pl.pallas_call(mm_kernel, grid=(m // tm, n // tn), in_specs=[pl.BlockSpec((tm, k), lambda i, j: (i, 0)), pl.BlockSpec((k, tn), lambda i, j: (0, j))],
        out_specs=pl.BlockSpec((tm, tn), lambda i, j: (i, j)), out_shape=jax.ShapeDtypeStruct((m, n), BF16), compiler_params=params(), cost_estimate=cost(2 * m * n * k))(x, w)

SQRT_HALF = 0.7071067811865476
INV_SQRT_2PI = 0.3989422804014327

def up_kernel(a_ref, w_ref, u_ref, h_ref):
    u = dot(a_ref[...].reshape(-1, a_ref.shape[-1]), w_ref[...]).astype(BF16)
    u_ref[...] = u.reshape(u_ref.shape)
    uf = u.astype(F32)
    h_ref[...] = (0.5 * uf * (1.0 + lax.erf(uf * SQRT_HALF))).astype(BF16).reshape(h_ref.shape)

def up(a3, w, half, tb, tn):
    b, s, d = a3.shape
    n = w.shape[1]
    hs = s // 2
    spec = pl.BlockSpec((tb, hs, tn), lambda i, j: (i, 0, j))
    return pl.pallas_call(up_kernel, grid=(b // tb, n // tn), in_specs=[pl.BlockSpec((tb, hs, d), lambda i, j: (i, half, 0)), pl.BlockSpec((d, tn), lambda i, j: (0, j))],
        out_specs=[spec, spec], out_shape=[jax.ShapeDtypeStruct((b, hs, n), BF16)] * 2, compiler_params=params(), name="up",
        cost_estimate=cost(2 * b * hs * n * d))(a3, w)

def gelu_grad(dy, w, u):
    dh = dot(dy, w, NT).astype(BF16).astype(F32)
    u = u.astype(F32)
    grad = 0.5 * (1.0 + lax.erf(u * SQRT_HALF)) + u * (jnp.exp(-0.5 * (u * u)) * INV_SQRT_2PI)
    return (dh * grad).astype(BF16)

def wgrad_qkv_kernel(a_ref, g_ref, z_ref, s_ref):
    bk = a_ref.shape[1]
    r = dot(a_ref[...], g_ref[...], TN)
    for n in range(2):
        for j in range(3):
            for t in range(2):
                c = (n * 3 + j) * 256 + t * 128
                s_ref[pl.ds(j * 4 + t * 2 + n, bk, stride=12), :] = r[:, c:c + 128]
    z_ref[...] = s_ref[...].astype(BF16)

def wgrad_qkv(a, g, bk=512):
    t, d = a.shape
    return pl.pallas_call(wgrad_qkv_kernel, grid=(d // bk,), in_specs=[pl.BlockSpec((t, bk), lambda i: (0, i)), pl.BlockSpec((t, 1536), lambda i: (0, 0))],
        out_specs=pl.BlockSpec((bk * 12, 128), lambda i: (i, 0)), out_shape=jax.ShapeDtypeStruct((d * 12, 128), BF16),
        scratch_shapes=[pltpu.VMEM((bk * 12, 128), F32)], compiler_params=params(), name="wgrad_qkv", cost_estimate=cost(2 * t * d * 1536))(a, g)

def att_probs(q, k, seg_c, seg_r):
    s = q.shape[0]
    sc = dot(q, k, NT) * (q.shape[1] ** -0.5)
    ok = (lax.broadcasted_iota(jnp.int32, (s, s), 1) <= lax.broadcasted_iota(jnp.int32, (s, s), 0)) & (seg_c == seg_r)
    sc = jnp.where(ok, sc, -1e30)
    e = jnp.exp(sc - jnp.max(sc, axis=-1, keepdims=True))
    return e / jnp.sum(e, axis=-1, keepdims=True)

def att_fwd_kernel(x_ref, segc_ref, segr_ref, o_ref):
    for n in range(2):
        q, k, v = (x_ref[0, :, (n * 3 + j) * 256:(n * 3 + j) * 256 + 256] for j in range(3))
        p = att_probs(q, k, segc_ref[0], segr_ref[0]).astype(BF16)
        o_ref[0, :, n * 256:n * 256 + 256] = dot(p, v).astype(BF16)

def att_fwd(qkv3, seg):
    b, s, c = qkv3.shape
    return pl.pallas_call(att_fwd_kernel, grid=(b,), in_specs=[pl.BlockSpec((1, s, c), lambda i: (i, 0, 0)),
        pl.BlockSpec((1, s, 1), lambda i: (i, 0, 0)), pl.BlockSpec((1, 1, s), lambda i: (i, 0, 0))],
        out_specs=pl.BlockSpec((1, s, 512), lambda i: (i, 0, 0)), out_shape=jax.ShapeDtypeStruct((b, s, 512), BF16),
        compiler_params=params(), name="att_fwd", cost_estimate=cost(8e9))(qkv3, seg[:, :, None], seg[:, None, :])

def att_bwd_kernel(x_ref, do_ref, segc_ref, segr_ref, dx_ref):
    for n in range(2):
        c = n * 768
        q, k, v = (x_ref[0, :, c + j * 256:c + j * 256 + 256] for j in range(3))
        do = do_ref[0, :, n * 256:n * 256 + 256]
        p = att_probs(q, k, segc_ref[0], segr_ref[0])
        dp = dot(do, v, NT)
        ds = (p * (dp - jnp.sum(dp * p, axis=-1, keepdims=True)) * (256 ** -0.5)).astype(BF16)
        dx_ref[0, :, c:c + 256] = dot(ds, k).astype(BF16)
        dx_ref[0, :, c + 256:c + 512] = dot(ds, q, TN).astype(BF16)
        dx_ref[0, :, c + 512:c + 768] = dot(p.astype(BF16), do, TN).astype(BF16)

def att_bwd(qkv3, do3, seg):
    b, s, c = qkv3.shape
    return pl.pallas_call(att_bwd_kernel, grid=(b,), in_specs=[pl.BlockSpec((1, s, c), lambda i: (i, 0, 0)), pl.BlockSpec((1, s, 512), lambda i: (i, 0, 0)),
        pl.BlockSpec((1, s, 1), lambda i: (i, 0, 0)), pl.BlockSpec((1, 1, s), lambda i: (i, 0, 0))],
        out_specs=pl.BlockSpec((1, s, c), lambda i: (i, 0, 0)), out_shape=jax.ShapeDtypeStruct((b, s, c), BF16),
        compiler_params=params(), name="att_bwd", cost_estimate=cost(12e9))(qkv3, do3, seg[:, :, None], seg[:, None, :])


MESH = pl.DeviceIdType.MESH


def rem(a, b):
    return lax.rem(a, jnp.int32(b))


class Stream:
    def __init__(self, source, slots, sems, count):
        self.source, self.slots, self.sems, self.count = source, slots, sems, count

    def start(self, t):
        self.source(t, self.slots.at[rem(t, 2)], self.sems.at[rem(t, 2)])

    def get(self, t, like):
        @pl.when(t + 1 < self.count)
        def _():
            self.start(t + 1)

        pltpu.make_async_copy(like, self.slots.at[rem(t, 2)], self.sems.at[rem(t, 2)]).wait()
        return self.slots.at[rem(t, 2)]


def product_scatter(cid, group, lhs, rhs, dims, hs, tn, lag, cover, finish, flops):
    chips = lhs[0][0].shape[0] // 2
    hid = rhs[0].shape[1 - dims[0][1][0]]
    t1, nl = hid // tn, len(lhs)
    total = t1 + cover['steps']
    assert total > t1 + lag
    halves = [half for _, half in lhs]
    lhs = [v.reshape(chips, 2, *v.shape[1:]) for v, _ in lhs]
    early = lambda i: jnp.minimum(i, t1 - 1)
    late = lambda i: jnp.maximum(i - t1, 0)
    anyspec = pl.BlockSpec(memory_space=pl.ANY)
    if dims is NN:
        w_specs = [pl.BlockSpec((w.shape[0], tn), lambda i: (0, early(i))) for w in rhs]
    else:
        w_specs = [pl.BlockSpec((tn, w.shape[1]), lambda i: (early(i), 0)) for w in rhs]
    shift = lambda sp: pl.BlockSpec(sp.block_shape, lambda i, m=sp.index_map: m(late(i)))
    cin, fin = cover['inputs'], finish['inputs']
    in_specs = [anyspec] * nl + w_specs + [anyspec] * (len(cin) + len(fin))
    out_specs = [shift(sp) for sp in cover['out_specs']] + finish['out_specs']
    nco, nfo = len(cover['out_specs']), len(finish['out_specs'])
    dma = pltpu.SemaphoreType.DMA
    comm = [pltpu.VMEM((2, chips, hs, tn), BF16), pltpu.VMEM((t1, chips, hs, tn), BF16), pltpu.VMEM((t1, chips, hs, tn), BF16),
            pltpu.VMEM((t1, hs, tn), BF16), pltpu.VMEM((t1, hs, tn), BF16), pltpu.VMEM((t1, hs, tn), BF16), dma((2,))] + [dma((t1,))] * 7
    left_bufs = [pltpu.VMEM((2, chips, hs, v.shape[3]), BF16) for v in lhs] + [dma((nl, 2))]

    def kernel(*refs):
        take = lambda n: (refs[:n], refs[n:])
        l_hbm, refs = take(nl)
        w_refs, refs = take(nl)
        ci, refs = take(len(cin))
        fi, refs = take(len(fin))
        co, refs = take(nco)
        fo, refs = take(nfo)
        (pair_out, pair_in, acc, fwd, from_left, from_right, s_pair, r_pair, s_far, r_far, s_left, s_right, r_left, r_right), refs = take(14)
        l_vmem, refs = take(nl)
        (l_sem,), refs = take(1)
        cs, fs = refs[:len(cover['scratch'])], refs[len(cover['scratch']):]
        i = pl.program_id(0)
        me = lax.axis_index('model')
        core = rem(me, 2)
        chip = lax.div(me, jnp.int32(2))
        c_right, c_left, c_far = rem(chip + 1, chips), rem(chip + chips - 1, chips), rem(chip + 2, chips)
        partner, to_right, to_left = me + 1 - 2 * core, c_right * 2 + core, c_left * 2 + core

        def remote(src, dst, ss, rs, dev):
            return pltpu.make_async_remote_copy(src_ref=src, dst_ref=dst, send_sem=ss, recv_sem=rs, device_id={'model': dev}, device_id_type=MESH)

        pair = lambda k: remote(pair_out.at[rem(k, 2)], pair_in.at[k], s_pair.at[rem(k, 2)], r_pair.at[k], partner)
        far = lambda k, dev: remote(acc.at[k, c_far], fwd.at[k], s_far.at[k], r_far.at[k], dev)
        leftward = lambda k: remote(acc.at[k, c_left], from_right.at[k], s_left.at[k], r_right.at[k], to_left)
        rightward = lambda k: remote(acc.at[k, c_right], from_left.at[k], s_right.at[k], r_left.at[k], to_right)

        def rows(x, core_slot, p):
            half = halves[x]
            return pltpu.make_async_copy(l_hbm[x].at[:, p, pl.ds(half * hs, hs)], l_vmem[x].at[core_slot], l_sem.at[x, core_slot])

        @pl.when(i == 0)
        def _():
            for x in range(nl):
                rows(x, 0, 1 - core).start()
            for x in range(nl):
                rows(x, 1, core).start()
            cover['begin'](ci, cs)
            finish['begin'](me, fi, fs)
            barrier = pltpu.get_barrier_semaphore()
            if finish['peers']:
                for j in range(1, group):
                    pl.semaphore_signal(barrier, inc=1, device_id={'model': rem(me + j, group)}, device_id_type=MESH)
                pl.semaphore_wait(barrier, group - 1)
            else:
                for dev in (partner, to_left, to_right):
                    pl.semaphore_signal(barrier, inc=1, device_id={'model': dev}, device_id_type=MESH)
                pl.semaphore_wait(barrier, 3)

        @pl.when((i >= 1) & (i <= t1))
        def _():
            k = i - 1
            pair(k).wait_recv()
            acc[k] = (acc[k].astype(F32) + pair_in[k].astype(F32)).astype(BF16)

            @pl.when(rem(k, 2) == 0)
            def _():
                far(k, to_right).start()
                leftward(k).start()

            @pl.when(rem(k, 2) == 1)
            def _():
                far(k, to_left).start()
                rightward(k).start()

        @pl.when((i >= 1 + lag) & (i <= t1 + lag))
        def _():
            k = i - 1 - lag
            far(k, to_right).wait_recv()

            @pl.when(rem(k, 2) == 0)
            def _():
                acc[k, c_right] = (acc[k, c_right].astype(F32) + fwd[k].astype(F32)).astype(BF16)
                rightward(k).start()

            @pl.when(rem(k, 2) == 1)
            def _():
                acc[k, c_left] = (acc[k, c_left].astype(F32) + fwd[k].astype(F32)).astype(BF16)
                leftward(k).start()

        @pl.when(i < t1)
        def _():
            def tile(slot):
                r = None
                for x, w in zip(l_vmem, w_refs):
                    v = dot(x[slot].reshape(chips * hs, x.shape[3]), w[...], dims)
                    r = v if r is None else r + v
                return r.astype(BF16).reshape(chips, hs, tn)

            @pl.when(i >= 2)
            def _():
                pair(i - 2).wait_send()

            @pl.when(i == 0)
            def _():
                for x in range(nl):
                    rows(x, 0, 1 - core).wait()

            pair_out[rem(i, 2)] = tile(0)
            pair(i).start()

            @pl.when(i == 0)
            def _():
                for x in range(nl):
                    rows(x, 1, core).wait()

            acc[i] = tile(1)

        @pl.when(i == t1 - 1)
        def _():
            cover['ready'](ci, cs)

        @pl.when(i >= t1)
        def _():
            cover['body'](i - t1, ci, co, cs)

        @pl.when(i == total - 1)
        def _():
            def drain(k, carry):
                far(k, to_right).wait_send()
                leftward(k).wait_send()
                rightward(k).wait_send()
                rightward(k).wait_recv()
                leftward(k).wait_recv()
                return carry

            for k in range(t1 - 2, t1):
                pair(jnp.int32(k)).wait_send()
            lax.fori_loop(jnp.int32(0), jnp.int32(t1), drain, jnp.int32(0))

            def summed(k, r0, nr):
                pick = lambda ref: ref[k, pl.ds(r0, nr)].astype(F32)
                return (acc[k, chip, pl.ds(r0, nr)].astype(F32) + pick(from_left) + pick(from_right)).astype(BF16).astype(F32)

            finish['end'](me, summed, t1, tn, fi, fo, fs)

    return pl.pallas_call(kernel, grid=(total,), in_specs=in_specs, out_specs=out_specs, out_shape=list(cover['out_shapes']) + list(finish['out_shapes']),
        scratch_shapes=comm + left_bufs + cover['scratch'] + finish['scratch'],
        compiler_params=params(63, collective_id=cid, has_side_effects=True), cost_estimate=cost(flops))(*lhs, *rhs, *cin, *fin)


def finish_y(x_in, half, hs):
    hid = x_in.shape[2]
    fetch = lambda me, fi, fs: pltpu.make_async_copy(fi[0].at[me, pl.ds(half * hs, hs)], fs[0], fs[1])

    def end(me, summed, t1, tn, fi, fo, fs):
        fetch(me, fi, fs).wait()
        for k in range(t1):
            fo[0][:, k * tn:(k + 1) * tn] = (fs[0][:, k * tn:(k + 1) * tn].astype(F32) + summed(k, 0, hs)).astype(BF16)

    return dict(inputs=[x_in], out_specs=[pl.BlockSpec((hs, hid), lambda i: (0, 0))], out_shapes=[jax.ShapeDtypeStruct((hs, hid), BF16)], peers=False,
        scratch=[pltpu.VMEM((hs, hid), BF16), pltpu.SemaphoreType.DMA(())], begin=lambda me, fi, fs: fetch(me, fi, fs).start(), end=end)


def finish_dx(x_in, dy_in, gain, group, nr=32):
    seq, hid = x_in.shape[1:]
    dma = pltpu.SemaphoreType.DMA

    def fetches(me, fi, fs):
        return [pltpu.make_async_copy(fi[0].at[me], fs[0], fs[4].at[0]), pltpu.make_async_copy(fi[1].at[me], fs[1], fs[4].at[1]), pltpu.make_async_copy(fi[2], fs[2], fs[4].at[2])]

    def begin(me, fi, fs):
        for c in fetches(me, fi, fs):
            c.start()

    def end(me, summed, t1, tn, fi, fo, fs):
        x_v, dy_v, g_v, dg_v, sems, s_dg, r_dg = fs
        for c in fetches(me, fi, fs):
            c.wait()
        g = g_v[...].astype(F32)

        def chunk(c, dg):
            r0 = pl.multiple_of(c * nr, nr)
            x = x_v[pl.ds(r0, nr)].astype(F32)
            cen = x - jnp.mean(x, axis=-1, keepdims=True)
            inv = lax.rsqrt(jnp.mean(cen * cen, axis=-1, keepdims=True) + LN_EPS)
            nf = cen * inv
            grad = jnp.concatenate([summed(k, r0, nr) for k in range(t1)], axis=1)
            dg = dg + jnp.sum(grad * nf, axis=0, keepdims=True)
            d_hat = grad * g
            d_x = inv * (d_hat - jnp.mean(d_hat, axis=-1, keepdims=True) - nf * jnp.mean(d_hat * nf, axis=-1, keepdims=True))
            x_v[pl.ds(r0, nr)] = (dy_v[pl.ds(r0, nr)].astype(F32) + d_x).astype(BF16)
            return dg

        dg_v[me] = lax.fori_loop(0, seq // nr, chunk, jnp.zeros((1, hid), F32))
        give = lambda slot, j, dev: pltpu.make_async_remote_copy(src_ref=dg_v.at[slot], dst_ref=dg_v.at[slot], send_sem=s_dg.at[j], recv_sem=r_dg.at[slot], device_id={'model': dev}, device_id_type=MESH)
        for j in range(1, group):
            give(me, j, rem(me + j, group)).start()
        out = pltpu.make_async_copy(x_v, fo[0], sems.at[0])
        out.start()
        for j in range(1, group):
            give(me, j, rem(me + j, group)).wait_send()
            give(rem(me + j, group), j, me).wait_recv()
        s = dg_v[0]
        for j in range(1, group):
            s = s + dg_v[j]
        fo[1][...] = s.astype(BF16)
        out.wait()

    return dict(inputs=[x_in, dy_in, gain.reshape(1, hid)], out_specs=[pl.BlockSpec(memory_space=pl.ANY), pl.BlockSpec((1, hid), lambda i: (0, 0))], peers=True,
        out_shapes=[jax.ShapeDtypeStruct((seq, hid), BF16), jax.ShapeDtypeStruct((1, hid), BF16)],
        scratch=[pltpu.VMEM((seq, hid), BF16), pltpu.VMEM((seq, hid), BF16), pltpu.VMEM((1, hid), BF16), pltpu.VMEM((group, 1, hid), F32), dma((3,)), dma((group,)), dma((group,))], begin=begin, end=end)


def share_up(cid, group, attn, h_a, wo, w_down, a3, w_up, x_in, tn=512, lag=3):
    b, s, d = a3.shape
    n, hs = w_up.shape[1], s // 2
    dma = pltpu.SemaphoreType.DMA
    lhs_copy = lambda ci, cs: pltpu.make_async_copy(ci[0].at[:, pl.ds(hs, hs)], cs[0], cs[1])
    stream = lambda ci, cs: Stream(lambda t, slot, sem: pltpu.make_async_copy(ci[1].at[:, pl.ds(pl.multiple_of(t * tn, tn), tn)], slot, sem).start(), cs[2], cs[3], n // tn)

    def body(t, ci, co, cs):
        @pl.when(t == 0)
        def _():
            lhs_copy(ci, cs).wait()

        w = stream(ci, cs).get(t, ci[1].at[:, pl.ds(0, tn)])
        up_kernel(cs[0], w, co[0], co[1])

    spec = pl.BlockSpec((b, hs, tn), lambda t: (0, 0, t))
    cover = dict(steps=n // tn, inputs=[a3, w_up], out_specs=[spec, spec], out_shapes=[jax.ShapeDtypeStruct((b, hs, n), BF16)] * 2, body=body,
        scratch=[pltpu.VMEM((b, hs, d), BF16), dma(()), pltpu.VMEM((2, d, tn), BF16), dma((2,))],
        begin=lambda ci, cs: lhs_copy(ci, cs).start(), ready=lambda ci, cs: stream(ci, cs).start(jnp.int32(0)))
    return product_scatter(cid, group, [(attn, 0), (h_a, 0)], [wo, w_down], NN, hs, tn, lag, cover, finish_y(x_in, 0, hs), 4e10)


def share_dh(cid, group, attn, h_b, wo, w_down, dy3, u_a, u_b, x_in, tn=512, lag=6):
    b, s, d = dy3.shape
    n, hs = w_down.shape[0], s // 2
    ko = wo.shape[0]
    assert ko == tn
    nt = n // tn
    per = nt + 1
    dma = pltpu.SemaphoreType.DMA
    dy_copy = lambda ci, cs, half: pltpu.make_async_copy(ci[0].at[:, pl.ds(half * hs, hs)], cs[0].at[half], cs[1].at[half])

    def w_source(ci):
        def go(t, slot, sem):
            j = rem(t, per)

            @pl.when(j < nt)
            def _():
                pltpu.make_async_copy(ci[1].at[pl.ds(pl.multiple_of(j * tn, tn), tn)], slot, sem).start()

            @pl.when(j == nt)
            def _():
                pltpu.make_async_copy(ci[2], slot, sem).start()

        return go

    def u_source(ci):
        def go(t, slot, sem):
            j, half = rem(t, nt), lax.div(t, jnp.int32(nt))
            for h in range(2):
                @pl.when(half == h)
                def _():
                    pltpu.make_async_copy(ci[3 + h].at[:, :, pl.ds(pl.multiple_of(j * tn, tn), tn)], slot, sem).start()

        return go

    w_stream = lambda ci, cs: Stream(w_source(ci), cs[2], cs[3], 2 * per)
    u_stream = lambda ci, cs: Stream(u_source(ci), cs[4], cs[5], 2 * nt)

    def begin(ci, cs):
        dy_copy(ci, cs, 0).start()

    def ready(ci, cs):
        w_stream(ci, cs).start(jnp.int32(0))
        u_stream(ci, cs).start(jnp.int32(0))
        dy_copy(ci, cs, 1).start()

    def body(t, ci, co, cs):
        half, j = lax.div(t, jnp.int32(per)), rem(t, per)
        for h in range(2):
            @pl.when(t == h * per)
            def _():
                dy_copy(ci, cs, h).wait()

        w = w_stream(ci, cs).get(t, ci[2])
        dy = lambda: cs[0][half].reshape(b * hs, d)

        @pl.when(j < nt)
        def _():
            u = u_stream(ci, cs).get(half * nt + j, ci[3].at[:, :, pl.ds(0, tn)])
            co[0][...] = gelu_grad(dy(), w[...], u[...].reshape(b * hs, tn)).reshape(b, hs, tn)

        @pl.when(j == nt)
        def _():
            co[1][...] = dot(dy(), w[...], NT).astype(BF16).reshape(b, hs, tn)

    cover = dict(steps=2 * per, inputs=[dy3, w_down, wo, u_a, u_b], body=body, begin=begin, ready=ready,
        out_specs=[pl.BlockSpec((b, hs, tn), lambda t: (0, t // per, jnp.minimum(t % per, nt - 1))), pl.BlockSpec((b, hs, ko), lambda t: (0, t // per, 0))],
        out_shapes=[jax.ShapeDtypeStruct((b, s, n), BF16), jax.ShapeDtypeStruct((b, s, ko), BF16)],
        scratch=[pltpu.VMEM((2, b, hs, d), BF16), dma((2,)), pltpu.VMEM((2, tn, d), BF16), dma((2,)), pltpu.VMEM((2, b, hs, tn), BF16), dma((2,))])
    return product_scatter(cid, group, [(attn, 1), (h_b, 0)], [wo, w_down], NN, hs, tn, lag, cover, finish_y(x_in, 1, hs), 7e10)


def dshare_wout(cid, group, d_qkv, d_up, wq, w_up, attn2, dy2, x_in, dy_in, gain, tn=512, tn2=256, lag=3):
    t, d = dy2.shape
    k = attn2.shape[1]
    dma = pltpu.SemaphoreType.DMA
    x_copy = lambda ci, cs: pltpu.make_async_copy(ci[0], cs[0], cs[1])
    stream = lambda ci, cs: Stream(lambda i, slot, sem: pltpu.make_async_copy(ci[1].at[:, pl.ds(pl.multiple_of(i * tn2, tn2), tn2)], slot, sem).start(), cs[2], cs[3], d // tn2)

    def body(i, ci, co, cs):
        @pl.when(i == 0)
        def _():
            x_copy(ci, cs).wait()

        g = stream(ci, cs).get(i, ci[1].at[:, pl.ds(0, tn2)])
        co[0][...] = dot(cs[0][...], g[...], TN).astype(BF16)

    cover = dict(steps=d // tn2, inputs=[attn2, dy2], body=body, begin=lambda ci, cs: x_copy(ci, cs).start(), ready=lambda ci, cs: stream(ci, cs).start(jnp.int32(0)),
        out_specs=[pl.BlockSpec((k, tn2), lambda i: (0, i))], out_shapes=[jax.ShapeDtypeStruct((k, d), BF16)],
        scratch=[pltpu.VMEM((t, k), BF16), dma(()), pltpu.VMEM((2, t, tn2), BF16), dma((2,))])
    return product_scatter(cid, group, [(d_qkv, 0), (d_up, 0)], [wq, w_up], NT, x_in.shape[1], tn, lag, cover, finish_dx(x_in, dy_in, gain, group), 8e10)


def wgrad_join(x, g, top, bottom, seq, tm, tn):
    k, m = x.shape
    n = g.shape[1]
    hid = top.shape[1]
    hs = seq // 2
    rows = top.shape[0] // hs
    cols = n // tn
    assert rows == (m // tm) * cols

    def body(x_ref, g_ref, t_ref, b_ref, o_ref, j_ref):
        o_ref[...] = dot(x_ref[...], g_ref[...], TN).astype(BF16)
        j_ref[0, :hs] = t_ref[...]
        j_ref[0, hs:] = b_ref[...]

    side = pl.BlockSpec((hs, hid), lambda i, j: (i * cols + j, 0))
    return pl.pallas_call(body, grid=(m // tm, cols), in_specs=[pl.BlockSpec((k, tm), lambda i, j: (0, i)), pl.BlockSpec((k, tn), lambda i, j: (0, j)), side, side],
        out_specs=[pl.BlockSpec((tm, tn), lambda i, j: (i, j)), pl.BlockSpec((1, seq, hid), lambda i, j: (i * cols + j, 0, 0))],
        out_shape=[jax.ShapeDtypeStruct((m, n), BF16), jax.ShapeDtypeStruct((rows, seq, hid), BF16)], compiler_params=params(), cost_estimate=cost(2 * m * n * k))(x, g, top, bottom)


def wgrad_halves(x_a, x_b, g3, tm, tn):
    b, hs, m = x_a.shape
    n = g3.shape[2]

    def body(xa_ref, xb_ref, g_ref, o_ref):
        rows = lambda v: v.reshape(b * hs, v.shape[2])
        o_ref[...] = (dot(rows(xa_ref[...]), rows(g_ref[:, :hs]), TN) + dot(rows(xb_ref[...]), rows(g_ref[:, hs:]), TN)).astype(BF16)

    x_spec = pl.BlockSpec((b, hs, tm), lambda i, j: (0, 0, i))
    return pl.pallas_call(body, grid=(m // tm, n // tn), in_specs=[x_spec, x_spec, pl.BlockSpec((b, 2 * hs, tn), lambda i, j: (0, 0, j))],
        out_specs=pl.BlockSpec((tm, tn), lambda i, j: (i, j)), out_shape=jax.ShapeDtypeStruct((m, n), BF16), compiler_params=params(), cost_estimate=cost(4 * m * n * b * hs))(x_a, x_b, g3)
from jax.sharding import PartitionSpec as P


def after(x, *deps):
    return lax.optimization_barrier((x, *deps))[0]


def solution(mesh):
    group = mesh.shape['model']

    def body(x_in, seg_ids, ln_gain, w_qkv, w_out, w_up, w_down, dy_in):
        rows, seq, hid = x_in.shape
        tok = rows * seq
        x2, dy2 = x_in.reshape(tok, hid), dy_in.reshape(tok, hid)
        three = lambda v: v.reshape(rows, seq, -1)
        wo = w_out.reshape(-1, hid)
        gather = lambda v: lax.all_gather(v, 'model', axis=0, tiled=True)
        wq = unpair(pair_view(w_qkv), bk=512)
        normed = layer_norm(x2, ln_gain, tm=512)
        qkv = matmul(normed, wq, 1024, 512)
        attn = att_fwd(three(qkv), seg_ids)
        u_a, h_a = up(three(normed), w_up, 0, 8, 512)
        u_b, h_b, y_a = share_up(1, group, attn, h_a, wo, w_down, three(normed), w_up, x_in)
        y_a = gather(y_a)
        d_up, d_attn, y_b = share_dh(2, group, attn, h_b, wo, w_down, dy_in, u_a, u_b, x_in)
        y_b = gather(y_b)
        d_qkv = att_bwd(three(qkv), d_attn, seg_ids)
        d_wout, dx, d_gain = dshare_wout(3, group, d_qkv, d_up, wq, w_up, attn.reshape(tok, -1), dy2, x_in, dy_in, ln_gain)
        dx_all = gather(dx)
        a_l = after(normed, dx)
        d_wdown = wgrad_halves(h_a, h_b, after(dy_in, dx), 1024, 1024)
        d_wqkv = unpair_view(wgrad_qkv(after(a_l, d_wdown), d_qkv.reshape(tok, -1)))
        d_wup, y_out = wgrad_join(after(a_l, d_wqkv), d_up.reshape(tok, -1), y_a, y_b, seq, 1024, 1024)
        return y_out, dx_all.reshape(x_in.shape), d_gain.reshape(hid), d_wqkv, d_wout.reshape(w_out.shape), d_wup, d_wdown

    in_specs = (P('data'), P('data'), P(), P(None, 'model'), P('model'), P(None, 'model'), P('model'), P('data'))
    out_specs = (P('data'), P('data'), P('data'), P('data', 'model'), P(('data', 'model')), P('data', 'model'), P(('data', 'model')))
    return jax.shard_map(body, mesh=mesh, in_specs=in_specs, out_specs=out_specs, check_vma=False)
```

```python
import jax
import jax.numpy as jnp
from jax import lax
from jax.experimental import pallas as pl
from jax.experimental.pallas import tpu as pltpu
from jax.sharding import PartitionSpec as P

F32, BF16, I32 = jnp.float32, jnp.bfloat16, jnp.int32
MESH = pl.DeviceIdType.MESH
ANY = pl.BlockSpec(memory_space=pl.ANY)
DMA = pltpu.SemaphoreType.DMA
VMEM = pltpu.VMEM
Spec = pl.BlockSpec
Shape = jax.ShapeDtypeStruct
LN_EPS = 1e-5
SQRT_HALF = 0.7071067811865476
INV_SQRT_2PI = 0.3989422804014327
LANES = 128
NN = (((1,), (0,)), ((), ()))
NT = (((1,), (1,)), ((), ()))
TN = (((0,), (0,)), ((), ()))
copy = pltpu.make_async_copy


def dot(x, w, dims=NN):
    return lax.dot_general(x, w, dims, preferred_element_type=F32)


def bf(x):
    return x.astype(BF16)


def f32(x):
    return x.astype(F32)


def rem(a, b):
    return lax.rem(a, I32(b))


def div(a, b):
    return lax.div(a, I32(b))


def span(k, size):
    return pl.ds(pl.multiple_of(k * size, size), size)


def flat(v):
    return v.reshape(-1, v.shape[-1])


def mean(x):
    return jnp.mean(x, axis=-1, keepdims=True)


def call(body, grid, in_specs, out_specs, out_shape, gflops, scratch=(), mib=60, **kw):
    return pl.pallas_call(body, grid=grid, in_specs=in_specs, out_specs=out_specs, out_shape=out_shape, scratch_shapes=list(scratch),
        cost_estimate=pl.CostEstimate(flops=gflops * 10**9, bytes_accessed=0, transcendentals=0), compiler_params=pltpu.CompilerParams(vmem_limit_bytes=mib << 20, **kw))


class Stream:
    def __init__(self, parts, slots, sems, count):
        self.parts, self.slots, self.sems, self.count = parts, slots, sems, count

    def copies(self, t):
        slot = rem(t, 2)
        return [copy(a, z, self.sems.at[slot, p]) for p, (a, z) in enumerate(self.parts(t, self.slots(slot)))]

    def start(self, t):
        for c in self.copies(t):
            c.start()

    def get(self, t):
        @pl.when(t + 1 < self.count)
        def _():
            self.start(t + 1)

        for c in self.copies(t):
            c.wait()
        return self.slots(rem(t, 2))


def pair_columns():
    for n in range(2):
        for j in range(3):
            for t in range(2):
                yield (j * 2 + t) * 2 + n, ((n * 3 + j) * 2 + t) * LANES


def pair_view(w):
    k, heads, three, d = w.shape
    return w.reshape(k, heads, three, d // LANES, LANES).transpose(0, 2, 3, 1, 4).reshape(-1, LANES)


def unpair_view(z, shape):
    k, heads, three, d = shape
    return z.reshape(k, three, d // LANES, heads, LANES).transpose(0, 3, 1, 2, 4).reshape(shape)


def norm_rows(x):
    cen = x - mean(x)
    return cen * lax.rsqrt(mean(cen * cen) + LN_EPS)


def gelu_of(u):
    u = f32(u)
    return bf(0.5 * u * (1.0 + lax.erf(u * SQRT_HALF)))


def probs(q, k, same):
    s, d = q.shape
    sc = dot(q, k, NT) * d ** -0.5
    sc = jnp.where(same, sc, -1e30)
    e = jnp.exp(sc - jnp.max(sc, axis=-1, keepdims=True))
    return e * (1.0 / jnp.sum(e, axis=-1, keepdims=True))


def allowed(seg_row):
    s = seg_row.shape[1]
    ids = jnp.broadcast_to(f32(seg_row), (s, s))
    return (lax.broadcasted_iota(I32, (s, s), 1) <= lax.broadcasted_iota(I32, (s, s), 0)) & (ids == ids.T)


def front(x_in, gain, w_up, z, seg, tn=512, nr=64, bk=256, ahead=4):
    b, s, d = x_in.shape
    n = w_up.shape[1]
    hs, steps = s // 2, n // tn
    wide = z.shape[0] // d
    nq = wide * LANES
    hd = nq // 6
    per = b // steps
    pieces = d // bk
    pp = pieces // steps

    def body(x_hbm, g_ref, w_hbm, z_hbm, seg_ref, a_hbm, wq_hbm, u_ref, h_ref, qkv_ref, o_ref, x_v, wq_v, w_v, z_v, s_v, sem_in, sem_out, sem_w, sem_z, sem_q):
        i = pl.program_id(0)
        fetch = lambda half, r: copy(x_hbm.at[r, pl.ds(half * hs, hs)], x_v.at[half, r], sem_in.at[half, r])
        give = lambda half, r: copy(x_v.at[half, r], a_hbm.at[r, pl.ds(half * hs, hs)], sem_out.at[half, r])
        z_in = lambda c: copy(z_hbm.at[span(c, bk * wide)], z_v.at[rem(c, ahead)], sem_z.at[rem(c, ahead)])
        w_stream = Stream(lambda t, slot: [(w_hbm.at[:, span(t, tn)], slot)], lambda slot: w_v.at[slot], sem_w, steps)
        q_out = lambda c: copy(wq_v.at[span(c, bk)], wq_hbm.at[span(c, bk)], sem_q.at[c])

        def norm(half, r):
            fetch(half, r).wait()
            g = f32(g_ref[:])

            def rows(c, _):
                at = span(c, nr)
                x_v[half, r, at] = bf(norm_rows(f32(x_v[half, r, at])) * g)
                return _

            lax.fori_loop(0, hs // nr, rows, 0)
            give(half, r).start()

        @pl.when(i == 0)
        def _():
            for r in range(ahead):
                fetch(0, r).start()
            w_stream.start(i)
            for c in range(ahead - 1):
                z_in(I32(c)).start()

        @pl.when(i < steps)
        def _():
            def norms(t, carry):
                @pl.when(t + ahead < 2 * b)
                def _():
                    fetch(div(t + ahead, b), rem(t + ahead, b)).start()

                norm(div(t, b), rem(t, b))
                return carry

            done = b + i * per
            lax.fori_loop(done * div(i + steps - 1, steps), done + per, norms, 0)
            u = bf(dot(flat(x_v[0]), w_stream.get(i)[:]))
            u_ref[:] = u.reshape(u_ref.shape)
            h_ref[:] = gelu_of(u).reshape(h_ref.shape)

            def unpair(q, carry):
                c = i * pp + q

                @pl.when(c + ahead - 1 < pieces)
                def _():
                    z_in(c + ahead - 1).start()

                z_in(c).wait()
                s_v[:] = f32(z_v[rem(c, ahead)])
                for row, col in pair_columns():
                    wq_v[span(c, bk), col:col + LANES] = bf(s_v[pl.ds(row, bk, stride=wide), :])
                q_out(c).start()
                return carry

            lax.fori_loop(0, pp, unpair, 0)

        @pl.when(i >= steps)
        def _():
            t = i - steps
            qkv = bf(dot(x_v[:, span(t, per)].reshape(2 * per * hs, d), wq_v[:])).reshape(2, per, hs, nq)
            for half in range(2):
                qkv_ref[:, half * hs:(half + 1) * hs] = qkv[half]

            def attend(r, _):
                same = allowed(seg_ref[pl.ds(t * per + r, 1)])
                for m in range(2):
                    c = m * 3 * hd
                    q, k, v = [qkv_ref[r, :, c + j * hd:c + (j + 1) * hd] for j in range(3)]
                    o_ref[r, :, m * hd:(m + 1) * hd] = bf(dot(bf(probs(q, k, same)), v))
                return _

            lax.fori_loop(0, per, attend, 0)

        @pl.when(i == 2 * steps - 1)
        def _():
            for half in range(2):
                for r in range(b):
                    give(half, r).wait()
            for c in range(pieces):
                q_out(c).wait()

    early = lambda i: jnp.minimum(i, steps - 1)
    late = lambda i: jnp.maximum(i - steps, 0)
    tile = Spec((b, hs, tn), lambda i: (0, 0, early(i)))
    seqs = lambda c: Spec((per, s, c), lambda i: (late(i), 0, 0))
    uh = Shape((b, hs, n), BF16)
    return call(body, (2 * steps,), [ANY, Spec((1, d), lambda i: (0, 0)), ANY, ANY, Spec((b, s), lambda i: (0, 0))],
        [ANY, ANY, tile, tile, seqs(nq), seqs(2 * hd)], [Shape((b, s, d), BF16), Shape((d, nq), BF16), uh, uh, Shape((b, s, nq), BF16), Shape((b, s, 2 * hd), BF16)], 60,
        [VMEM((2, b, hs, d), BF16), VMEM((d, nq), BF16), VMEM((2, d, tn), BF16), VMEM((ahead, bk * wide, LANES), BF16), VMEM((bk * wide, LANES), F32), DMA((2, b)), DMA((2, b)), DMA((2, 1)), DMA((ahead,)), DMA((pieces,))], 63)(x_in, gain, w_up, z, seg)


def attention_grad(qkv, grads, seg):
    b, s, c = qkv.shape
    d = c // 6
    last = grads.shape[2] // (2 * d) - 1

    def body(x_ref, do_ref, seg_ref, dx_ref):
        same = allowed(seg_ref[pl.ds(pl.program_id(0), 1)])
        for m in range(2):
            c0 = m * 3 * d
            q, k, v = [x_ref[0, :, c0 + j * d:c0 + (j + 1) * d] for j in range(3)]
            g = do_ref[0, :, m * d:(m + 1) * d]
            p = probs(q, k, same)
            dp = dot(g, v, NT)
            ds = bf(p * (dp - jnp.sum(dp * p, axis=-1, keepdims=True)) * d ** -0.5)
            for j, r in enumerate((dot(ds, k), dot(ds, q, TN), dot(bf(p), g, TN))):
                dx_ref[0, :, c0 + j * d:c0 + (j + 1) * d] = bf(r)

    row = lambda w: Spec((1, s, w), lambda i: (i, 0, 0))
    return call(body, (b,), [row(c), Spec((1, s, 2 * d), lambda i: (i, 0, last)), Spec((b, s), lambda i: (0, 0))], row(c), Shape((b, s, c), BF16), 12)(qkv, grads, seg)


def product_scatter(cid, group, lhs, rhs, dims, hs, tn, relay, cover, finish, gflops, pair_lag=2):
    chips = lhs[0][0].shape[0] // 2
    nt = dims is NT
    hid = rhs[0].shape[0 if nt else 1]
    depths = [w.shape[1 if nt else 0] for w in rhs]
    at = [sum(depths[:x]) for x in range(len(lhs) + 1)]
    depth = at[-1]
    t1, nl = hid // tn, len(lhs)
    total = t1 + cover['steps']
    first, stride = relay
    assert first > pair_lag and first + stride * (t1 - 1) < total
    halves = [half for _, half in lhs]
    lhs = [v.reshape(chips, 2, *v.shape[1:]) for v, _ in lhs]
    late = lambda sp: Spec(sp.block_shape, lambda i: sp.index_map(jnp.maximum(i - t1, 0)))
    cin, fin = cover['inputs'], finish['inputs']
    out_specs = [late(sp) for sp in cover['out_specs']] + finish['out_specs']
    tiles = lambda count: VMEM((count, chips, hs, tn), BF16)
    part = VMEM((t1, hs, tn), BF16)
    scratch = [tiles(t1), tiles(t1 + 2), part, part, part, DMA((2,))] + [DMA((t1,))] * 7
    scratch += [VMEM((2, chips, hs, depth), BF16), DMA((2, nl)), VMEM((2, tn, depth) if nt else (2, depth, tn), BF16), DMA((2, nl))]

    def kernel(*refs):
        refs = list(refs)
        take = lambda n: [refs.pop(0) for _ in range(n)]
        l_hbm, w_hbm, ci, fi = take(nl), take(nl), take(len(cin)), take(len(fin))
        co, fo = take(len(cover['out_specs'])), take(len(finish['out_specs']))
        pair_in, acc, fwd, from_left, from_right, s_pair, r_pair, s_far, r_far, s_left, s_right, r_left, r_right = take(13)
        l_v, l_sem, w_v, w_sem = take(4)
        cs, fs = take(len(cover['scratch'])), refs
        i = pl.program_id(0)
        me = lax.axis_index('model')
        core, chip = rem(me, 2), div(me, 2)
        c_right, c_left, c_far = rem(chip + 1, chips), rem(chip + chips - 1, chips), rem(chip + 2, chips)
        partner, to_right, to_left = me + 1 - 2 * core, c_right * 2 + core, c_left * 2 + core

        def remote(src, dst, ss, rs, dev):
            return pltpu.make_async_remote_copy(src_ref=src, dst_ref=dst, send_sem=ss, recv_sem=rs, device_id={'model': dev}, device_id_type=MESH)

        pair = lambda k: remote(acc.at[t1 + rem(k, 2)], pair_in.at[k], s_pair.at[rem(k, 2)], r_pair.at[k], partner)
        far = lambda k, dev: remote(acc.at[k, c_far], fwd.at[k], s_far.at[k], r_far.at[k], dev)
        leftward = lambda k: remote(acc.at[k, c_left], from_right.at[k], s_left.at[k], r_right.at[k], to_left)
        rightward = lambda k: remote(acc.at[k, c_right], from_left.at[k], s_right.at[k], r_left.at[k], to_right)
        rows = lambda x, slot, p: copy(l_hbm[x].at[:, p, pl.ds(halves[x] * hs, hs), :depths[x]], l_v.at[slot, :, :, at[x]:at[x + 1]], l_sem.at[slot, x])

        def w_parts(t, slot):
            if nt:
                return [(w.at[span(t, tn)], slot.at[:, at[x]:at[x + 1]]) for x, w in enumerate(w_hbm)]
            return [(w.at[:, span(t, tn)], slot.at[at[x]:at[x + 1]]) for x, w in enumerate(w_hbm)]

        w_stream = Stream(w_parts, lambda slot: w_v.at[slot], w_sem, t1)

        def each(k, even, odd):
            for want, go in ((0, even), (1, odd)):
                @pl.when(rem(k, 2) == want)
                def _():
                    go()

        @pl.when(i == 0)
        def _():
            for x in range(nl):
                rows(x, 0, 1 - core).start()
            w_stream.start(i)
            for x in range(nl):
                rows(x, 1, core).start()
            barrier = pltpu.get_barrier_semaphore()
            peers = [rem(me + j, group) for j in range(1, group)] if finish['peers'] else [partner, to_left, to_right]
            for dev in peers:
                pl.semaphore_signal(barrier, inc=1, device_id={'model': dev}, device_id_type=MESH)
            pl.semaphore_wait(barrier, len(peers))

        @pl.when(i == 1)
        def _():
            cover['begin'](ci, cs)
            finish['begin'](me, fi, fs)

        @pl.when((i >= pair_lag) & (i < t1 + pair_lag))
        def _():
            k = i - pair_lag
            pair(k).wait_recv()
            acc[k] = acc[k] + pair_in[k]

            def even():
                far(k, to_right).start()
                leftward(k).start()

            def odd():
                far(k, to_left).start()
                rightward(k).start()

            each(k, even, odd)

        @pl.when((i >= first) & (i < first + stride * t1) & (rem(i - first, stride) == 0))
        def _():
            k = div(i - first, stride)
            far(k, to_right).wait_recv()

            def even():
                acc[k, c_right] = acc[k, c_right] + fwd[k]
                rightward(k).start()

            def odd():
                acc[k, c_left] = acc[k, c_left] + fwd[k]
                leftward(k).start()

            each(k, even, odd)

        @pl.when(i < t1)
        def _():
            w = w_stream.get(i)

            @pl.when(i >= 2)
            def _():
                pair(i - 2).wait_send()

            def tile(slot, carry):
                @pl.when(i == 0)
                def _():
                    for x in range(nl):
                        rows(x, slot, core * slot + (1 - core) * (1 - slot)).wait()

                acc[i * slot + (t1 + rem(i, 2)) * (1 - slot)] = bf(dot(l_v[slot].reshape(chips * hs, depth), w[:], dims)).reshape(chips, hs, tn)

                @pl.when(slot == 0)
                def _():
                    pair(i).start()

                return carry

            lax.fori_loop(I32(0), I32(2), tile, I32(0))

        @pl.when(i == t1 - 1)
        def _():
            cover['ready'](ci, cs, l_v)

        @pl.when(i >= t1)
        def _():
            cover['body'](i - t1, ci, co, cs, l_v)

        @pl.when(i == total - 1)
        def _():
            def drain(k, _):
                far(k, to_right).wait_send()
                for c in (leftward(k), rightward(k)):
                    c.wait_send()
                    c.wait_recv()
                return _

            for k in range(t1 - 2, t1):
                pair(I32(k)).wait_send()
            lax.fori_loop(I32(0), I32(t1), drain, I32(0))
            summed = lambda k, r: f32(bf(f32(acc[k, chip, r]) + f32(from_left[k, r]) + f32(from_right[k, r])))
            finish['end'](me, summed, t1, tn, fi, fo, fs)

    return call(kernel, (total,), [ANY] * (2 * nl + len(cin) + len(fin)), out_specs, list(cover['out_shapes']) + list(finish['out_shapes']), gflops,
        scratch + cover['scratch'] + finish['scratch'], 63, collective_id=cid, has_side_effects=True)(*lhs, *rhs, *cin, *fin)


def finish_y(x_in, half, hs):
    hid = x_in.shape[2]
    fetch = lambda me, fi, fs: copy(fi[0].at[me, pl.ds(half * hs, hs)], fs[0], fs[1])

    def end(me, summed, t1, tn, fi, fo, fs):
        fetch(me, fi, fs).wait()
        for k in range(t1):
            at = slice(k * tn, (k + 1) * tn)
            fo[0][:, at] = bf(f32(fs[0][:, at]) + summed(k, slice(None)))

    return dict(inputs=[x_in], out_specs=[Spec((hs, hid), lambda i: (0, 0))], out_shapes=[Shape((hs, hid), BF16)], peers=False,
        scratch=[VMEM((hs, hid), BF16), DMA(())], begin=lambda me, fi, fs: fetch(me, fi, fs).start(), end=end)


def finish_dx(x_in, dy_in, gain, group, tn=512, nr=32):
    seq, hid = x_in.shape[1:]
    t1 = hid // tn

    def fetches(me, fi, fs):
        return [copy(src, fs[x], fs[4].at[x]) for x, src in enumerate((fi[0].at[me], fi[1].at[me], fi[2]))]

    def begin(me, fi, fs):
        for c in fetches(me, fi, fs):
            c.start()

    def end(me, summed, t1, tn, fi, fo, fs):
        x_v, dy_v, g_v, dg_v, sems, s_dg, r_dg, part_v, grad_v = fs
        for c in fetches(me, fi, fs):
            c.wait()
        cols = [slice(k * tn, (k + 1) * tn) for k in range(t1)]
        whole = lambda v: jnp.sum(v, axis=-1, keepdims=True) * (1.0 / hid)
        part_v[:] = jnp.zeros(part_v.shape, F32)

        def chunk(c, _):
            at = span(c, nr)
            x = lambda k: f32(x_v[at, cols[k]])
            mu = whole(sum(x(k) for k in range(t1)))
            var = whole(sum((x(k) - mu) * (x(k) - mu) for k in range(t1)))
            inv = lax.rsqrt(var + LN_EPS)
            m1 = m2 = 0.0
            for k in range(t1):
                nf = (x(k) - mu) * inv
                grad = summed(k, at)
                grad_v[:, cols[k]] = grad
                part_v[k] += jnp.sum((grad * nf).reshape(nr // 8, 8, tn), axis=0)
                hat = grad * f32(g_v[:, cols[k]])
                m1, m2 = m1 + hat, m2 + hat * nf
            m1, m2 = whole(m1), whole(m2)
            for k in range(t1):
                hat = grad_v[:, cols[k]] * f32(g_v[:, cols[k]])
                x_v[at, cols[k]] = bf(f32(dy_v[at, cols[k]]) + inv * (hat - m1 - (x(k) - mu) * inv * m2))
            return _

        lax.fori_loop(0, seq // nr, chunk, 0)
        dg_v[me] = jnp.sum(part_v[:], axis=1)
        give = lambda slot, j, dev: pltpu.make_async_remote_copy(src_ref=dg_v.at[slot], dst_ref=dg_v.at[slot], send_sem=s_dg.at[j], recv_sem=r_dg.at[slot], device_id={'model': dev}, device_id_type=MESH)
        for j in range(1, group):
            give(me, j, rem(me + j, group)).start()
        out = copy(x_v, fo[0], sems.at[0])
        out.start()
        for j in range(1, group):
            give(me, j, rem(me + j, group)).wait_send()
            give(rem(me + j, group), j, me).wait_recv()
        fo[1][:] = bf(sum(dg_v[j] for j in range(group)))
        out.wait()

    rows = VMEM((seq, hid), BF16)
    return dict(inputs=[x_in, dy_in, gain], out_specs=[ANY, Spec((t1, tn), lambda i: (0, 0))], peers=True, out_shapes=[Shape((seq, hid), BF16), Shape((t1, tn), BF16)],
        scratch=[rows, rows, VMEM((1, hid), BF16), VMEM((group, t1, tn), F32), DMA((3,)), DMA((group,)), DMA((group,)), VMEM((t1, 8, tn), F32), VMEM((nr, hid), F32)], begin=begin, end=end)


def share_up(cid, group, attn, h_a, wo, w_down, a3, w_up, x_in, tn=512, relay=(4, 1)):
    b, s, d = a3.shape
    n, hs = w_up.shape[1], s // 2
    lhs_copy = lambda ci, cs: copy(ci[0].at[:, pl.ds(hs, hs)], cs[0], cs[1])
    stream = lambda ci, cs: Stream(lambda t, slot: [(ci[1].at[:, span(t, tn)], slot)], lambda slot: cs[2].at[slot], cs[3], n // tn)

    def body(t, ci, co, cs, _):
        @pl.when(t == 0)
        def _():
            lhs_copy(ci, cs).wait()

        w = stream(ci, cs).get(t)
        u = bf(dot(flat(cs[0][:]), w[:]))
        co[0][:] = u.reshape(b, hs, tn)
        co[1][:] = gelu_of(u).reshape(b, hs, tn)

    tile = Spec((b, hs, tn), lambda t: (0, 0, t))
    cover = dict(steps=n // tn, inputs=[a3, w_up], out_specs=[tile, tile], out_shapes=[Shape((b, hs, n), BF16)] * 2, body=body,
        scratch=[VMEM((b, hs, d), BF16), DMA(()), VMEM((2, d, tn), BF16), DMA((2, 1))],
        begin=lambda ci, cs: lhs_copy(ci, cs).start(), ready=lambda ci, cs, _: stream(ci, cs).start(I32(0)))
    return product_scatter(cid, group, [(attn, 0), (h_a, 0)], [wo, w_down], NN, hs, tn, relay, cover, finish_y(x_in, 0, hs), 40)


def share_dh(cid, group, attn, h_b, wo, w_down, dy3, u_a, u_b, x_in, tn=512, relay=(7, 1)):
    b, s, d = dy3.shape
    n, hs = w_down.shape[0], s // 2
    ko = wo.shape[0]
    assert ko == tn
    nt = n // tn
    per = nt + 1
    dy_copy = lambda ci, cs, half: copy(ci[0].at[:, pl.ds(half * hs, hs)], cs[0].at[half], cs[1].at[half])
    w_all = lambda ci, cs: [Stream(lambda t, slot, src=src: [(src(t), slot)], lambda slot: cs[2].at[slot], cs[3], 2 * per) for src in (lambda t: ci[1].at[span(rem(t, per), tn)], lambda t: ci[2])]
    u_all = lambda ci, cs: [Stream(lambda t, slot, src=src: [(src.at[:, :, span(rem(t, nt), tn)], slot)], lambda slot: cs[4].at[slot], cs[5], 2 * nt) for src in ci[3:]]

    def w_start(ci, cs, t):
        for last, st in enumerate(w_all(ci, cs)):
            @pl.when((rem(t, per) == nt) == bool(last))
            def _():
                st.start(t)

    def u_start(ci, cs, t):
        for half, st in enumerate(u_all(ci, cs)):
            @pl.when(div(t, nt) == half)
            def _():
                st.start(t)

    def ready(ci, cs, _):
        w_start(ci, cs, I32(0))
        u_start(ci, cs, I32(0))
        dy_copy(ci, cs, 1).start()

    def body(t, ci, co, cs, _):
        half, j = div(t, per), rem(t, per)
        for h in range(2):
            @pl.when(t == h * per)
            def _():
                dy_copy(ci, cs, h).wait()

        @pl.when(t + 1 < 2 * per)
        def _():
            w_start(ci, cs, t + 1)

        w_all(ci, cs)[1].copies(t)[0].wait()
        w = cs[2][rem(t, 2)]

        v = half * nt + jnp.minimum(j, nt - 1)

        @pl.when((j < nt) & (v + 1 < 2 * nt))
        def _():
            u_start(ci, cs, v + 1)

        @pl.when(j < nt)
        def _():
            u_all(ci, cs)[0].copies(v)[0].wait()

        u = f32(flat(cs[4][rem(v, 2)]))
        grad = 0.5 * (1.0 + lax.erf(u * SQRT_HALF)) + u * (jnp.exp(-0.5 * (u * u)) * INV_SQRT_2PI)
        grad = jnp.where(j < nt, grad, 1.0)
        co[0][:] = bf(f32(bf(dot(flat(cs[0][half]), w, NT))) * grad).reshape(b, hs, tn)

    cover = dict(steps=2 * per, inputs=[dy3, w_down, wo, u_a, u_b], body=body, begin=lambda ci, cs: dy_copy(ci, cs, 0).start(), ready=ready,
        out_specs=[Spec((b, hs, tn), lambda t: (0, t // per, t % per))], out_shapes=[Shape((b, s, n + ko), BF16)],
        scratch=[VMEM((2, b, hs, d), BF16), DMA((2,)), VMEM((2, tn, d), BF16), DMA((2, 1)), VMEM((2, b, hs, tn), BF16), DMA((2, 1))])
    return product_scatter(cid, group, [(attn, 1), (h_b, 0)], [wo, w_down], NN, hs, tn, relay, cover, finish_y(x_in, 1, hs), 70)


def dshare_wgrad(cid, group, d_qkv, d_up, wq, w_up, h_a, h_b, attn, dy_in, x_in, gain, tn=512, relay=(8, 3), tm2=1024, tn2=512):
    b, s, d = dy_in.shape
    n, ko = h_a.shape[2], attn.shape[2]
    hs, cols, wide = s // 2, d // tn2, n // tm2
    x_at = [t * tm2 for t in range(wide)] + [n, n + ko]
    main = wide * cols
    four = lambda v: v.reshape(b // 2, 2, *v.shape[1:])

    def x_copies(ci, cs, lv, t):
        to = lambda p, r: lv.at[p, :, r, x_at[t]:x_at[t + 1]]
        if t == wide:
            return [copy(ci[2].at[:, p], to(p, slice(None)), cs[0].at[t, p, 0]) for p in range(2)]
        return [copy(ci[h].at[:, p, :, x_at[t]:x_at[t] + tm2], to(p, pl.ds(h * hs, hs)), cs[0].at[t, p, h]) for p in range(2) for h in range(2)]

    def g_stream(ci, cs, lv):
        lo = n + ko
        slots = lambda slot: pl.ds(pl.multiple_of(lo + slot * tn2, tn2), tn2)
        return Stream(lambda t, at: [(ci[3].at[:, p, :, span(rem(t, cols), tn2)], lv.at[p, :, :, at]) for p in range(2)], slots, cs[1], main + cols)

    def ready(ci, cs, lv):
        for c in x_copies(ci, cs, lv, 0):
            c.start()
        g_stream(ci, cs, lv).start(I32(0))
        for t in range(1, wide + 1):
            for c in x_copies(ci, cs, lv, t):
                c.start()

    def body(t, ci, co, cs, lv):
        for x in range(wide + 1):
            @pl.when(t == x * cols)
            def _():
                for c in x_copies(ci, cs, lv, x):
                    c.wait()

        g = lv[:, :, :, g_stream(ci, cs, lv).get(t)].reshape(-1, tn2)

        @pl.when(t < main)
        def _():
            co[0][:] = bf(dot(lv[:, :, :, span(div(t, cols), tm2)].reshape(-1, tm2), g, TN))

        @pl.when(t >= main)
        def _():
            co[1][:] = bf(dot(lv[:, :, :, n:n + ko].reshape(-1, ko), g, TN))

    cover = dict(steps=main + cols, inputs=[four(h_a), four(h_b), four(attn), four(dy_in)], body=body, begin=lambda ci, cs: None, ready=ready,
        out_specs=[Spec((tm2, tn2), lambda t: (jnp.minimum(t, main - 1) // cols, jnp.minimum(t, main - 1) % cols)), Spec((ko, tn2), lambda t: (0, jnp.maximum(t - main, 0)))],
        out_shapes=[Shape((n, d), BF16), Shape((ko, d), BF16)], scratch=[DMA((wide + 1, 2, 2)), DMA((2, 2))])
    return product_scatter(cid, group, [(d_qkv, 0), (d_up, 0)], [wq, w_up], NT, s, tn, relay, cover, finish_dx(x_in, dy_in, gain, group), 100)


def wgrad_in(a, d_qkv, d_up, top, bottom, d_wdown, d_wout, seq, bk=512):
    t, d = a.shape
    nq, nu = d_qkv.shape[1], d_wdown.shape[0]
    wide, steps = nq // LANES, d // bk
    hs, rows = seq // 2, top.shape[0] * 2 // seq
    assert rows == steps
    rd, ro = d_wdown.shape[0] // steps, d_wout.shape[0] // steps

    def body(a_ref, gq_ref, gu_hbm, top_h, bot_h, dn_h, wo_h, z_ref, o_ref, y_h, dno_h, woo_h, s_v, gu_v, gu_sem, buf, sem_in, sem_out):
        i = pl.program_id(0)
        fetch_gu = copy(gu_hbm.at[:, :nu], gu_v, gu_sem)

        def moves(k):
            lo, slot = seq + rd, rem(k, 2)
            parts = [(top_h.at[span(k, hs)], y_h.at[k, pl.ds(0, hs)], 0, hs), (bot_h.at[span(k, hs)], y_h.at[k, pl.ds(hs, hs)], hs, seq),
                     (dn_h.at[span(k, rd)], dno_h.at[span(k, rd)], seq, lo), (wo_h.at[span(k, ro)], woo_h.at[span(k, ro)], lo, lo + ro)]
            return [(copy(src, buf.at[slot, p:q], sem_in.at[slot, m]), copy(buf.at[slot, p:q], dst, sem_out.at[slot, m])) for m, (src, dst, p, q) in enumerate(parts)]

        def put(k):
            for c, o in moves(k):
                c.wait()
                o.start()

        def done(k):
            for _, o in moves(k):
                o.wait()

        @pl.when(i == 0)
        def _():
            fetch_gu.start()

        @pl.when(i >= 1)
        def _():
            put(i - 1)

        @pl.when(i >= 2)
        def _():
            done(i - 2)

        for c, _ in moves(i):
            c.start()
        x = a_ref[:]
        r = dot(x, gq_ref[:], TN)
        for row, col in pair_columns():
            s_v[pl.ds(row, bk, stride=wide), :] = r[:, col:col + LANES]
        z_ref[:] = bf(s_v[:])

        @pl.when(i == 0)
        def _():
            fetch_gu.wait()

        o_ref[:] = bf(dot(x, gu_v[:], TN))

        @pl.when(i == steps - 1)
        def _():
            done(i - 1)
            put(i)
            done(i)

    outs = [Shape((d * wide, LANES), BF16), Shape((d, nu), BF16), Shape((rows, seq, d), BF16), Shape(d_wdown.shape, BF16), Shape(d_wout.shape, BF16)]
    return call(body, (steps,), [Spec((t, bk), lambda i: (0, i)), Spec((t, nq), lambda i: (0, 0), pipeline_mode=pl.Buffered(1))] + [ANY] * 5,
        [Spec((bk * wide, LANES), lambda i: (i, 0)), Spec((bk, nu), lambda i: (i, 0)), ANY, ANY, ANY], outs, 66,
        [VMEM((bk * wide, LANES), F32), VMEM((t, nu), BF16), DMA(()), VMEM((2, seq + rd + ro, d), BF16), DMA((2, 4)), DMA((2, 4))])(a, d_qkv, d_up, top, bottom, d_wdown, d_wout)


def moved(x, rows=512, depth=4):
    m, n = x.shape
    count = m // rows

    def body(x_h, o_h, buf, sem_in, sem_out):
        load = lambda k: copy(x_h.at[pl.ds(k * rows, rows)], buf.at[k % depth], sem_in.at[k % depth])
        store = lambda k: copy(buf.at[k % depth], o_h.at[pl.ds(k * rows, rows)], sem_out.at[k % depth])
        for k in range(min(depth, count)):
            load(k).start()
        for k in range(count):
            load(k).wait()
            store(k).start()
            if k + depth < count:
                store(k).wait()
                load(k + depth).start()
        for k in range(max(0, count - depth), count):
            store(k).wait()

    return call(body, (), [ANY], ANY, Shape((m, n), BF16), 1, [VMEM((depth, rows, n), BF16), DMA((depth,)), DMA((depth,))])(x)


def after(x, *deps):
    return lax.optimization_barrier((x, *deps))[0]


def solution(mesh):
    group = mesh.shape['model']

    def body(x_in, seg_ids, ln_gain, w_qkv, w_out, w_up, w_down, dy_in):
        rows, seq, hid = x_in.shape
        wo = w_out.reshape(-1, hid)
        gain = ln_gain.reshape(1, hid)
        gather = lambda v: lax.all_gather(v, 'model', axis=0, tiled=True)
        normed, wq, u_a, h_a, qkv, attn = front(x_in, gain, w_up, pair_view(w_qkv), seg_ids)
        u_b, h_b, y_a = share_up(1, group, attn, h_a, wo, w_down, normed, w_up, x_in)
        y_a = gather(y_a)
        grads, y_b = share_dh(2, group, attn, h_b, wo, w_down, dy_in, u_a, u_b, x_in)
        y_b = gather(y_b)
        d_qkv = attention_grad(qkv, grads, seg_ids)
        d_wdown, d_wout, dx, d_gain = dshare_wgrad(3, group, d_qkv, grads, wq, w_up, h_a, h_b, attn, dy_in, x_in, gain)
        dx_all = gather(dx)
        z, d_wup, y_out, d_wdown, d_wout = wgrad_in(after(flat(normed), dx), flat(d_qkv), flat(grads), y_a, y_b, d_wdown, d_wout, seq)
        return y_out, moved(dx_all).reshape(x_in.shape), d_gain.reshape(hid), unpair_view(z, w_qkv.shape), d_wout.reshape(w_out.shape), d_wup, d_wdown

    in_specs = (P('data'), P('data'), P(), P(None, 'model'), P('model'), P(None, 'model'), P('model'), P('data'))
    out_specs = (P('data'), P('data'), P('data'), P('data', 'model'), P(('data', 'model')), P('data', 'model'), P(('data', 'model')))
    return jax.shard_map(body, mesh=mesh, in_specs=in_specs, out_specs=out_specs, check_vma=False)
```
